256 devices in a mesh: scen: 64 (over z, y, core), cell: 2 (over x_hi), site: 2 (over x_lo).
Axes of the slice: x: 4 (x_hi: 2, x_lo: 2; x = x_hi * 2 + x_lo), y: 4, z: 8, core: 2. Of those that a mesh axis runs over, the one named last changes fastest.
Arguments:
- demand: float32 [64, 2048], P('scen', 'cell'), may hold values from 0.1 to 10
- start_potential: float32 [64, 16384], P('scen', 'site'), may hold values from -60 to 60
- cell_feat: bfloat16 [32, 2048], P(None, ('cell', 'scen', 'site')), may hold values from -8 to 8
- site_feat: bfloat16 [32, 16384], P(None, 'site'), may hold values from -8 to 8
- weights: float32 [64], replicated, may hold values from 0.5 to 4
Outputs:
- cell_potential: float32 [64, 2048], P('scen', 'cell')
- site_potential: float32 [64, 16384], P('scen', 'site')
- log_barycenter: float32 [16384], P('site')
The draws below stay inside these ranges and needn't reach their ends.
All inputs are finite; a program needn't handle non-finite values.
Results may differ from the reference program's by a relative error of at most 0.0003.
Values may be sent and summed in bfloat16 or wider, within the bound.
No kernel may reach another device: no remote copies, remote signals or barrier semaphores. Data moves between devices by JAX's collectives and lax.ppermute only.
A program may use at most 128 MiB of HBM per device.

```python
import math
import jax
import jax.numpy as jnp
from jax import lax

D = 32
CELL_DEV = 1024
ITERS = 2
SCEN = 64
CELLS = 2048
SITES = 16384


def draw_cell_feat(key, part):
    values = jnp.clip(jax.random.normal(jax.random.fold_in(key, 5), (D, CELLS), jnp.float32), -4.0, 4.0)
    return values.astype(jnp.bfloat16)


def draw_site_feat(key, part):
    values = jnp.clip(jax.random.normal(jax.random.fold_in(key, 6), (D, SITES), jnp.float32), -4.0, 4.0)
    return values.astype(jnp.bfloat16)


def draw_start_potential(key, part):
    values = 0.5 * jax.random.normal(jax.random.fold_in(key, 9), (SCEN, SITES), jnp.float32)
    return values


def shard_levels(rng, shape, cuts, smallest, high):
    factor_of = 1.0
    for dim, shards_of in cuts:
        steps = jax.random.uniform(jax.random.fold_in(jax.random.fold_in(rng, 6), dim), (shards_of,), jnp.float32, smallest / len(cuts), high / len(cuts))
        factor_of = factor_of * jnp.repeat(jnp.exp(steps), shape[dim] // shards_of).reshape((-1,) + (1,) * (len(shape) - 1 - dim))
    return factor_of


def setup_inputs(seed: int = 0) -> dict:
    seeds = jax.random.split(jax.random.key(seed), 6)
    demand = jnp.clip(jnp.exp(math.log(10.0) - 4.6051702 * jax.random.uniform(seeds[0], (SCEN, CELLS), jnp.float32) ** shard_levels(seeds[0], (SCEN, CELLS), ((0, 64), (1, 2)), -0.2, 0.2)), 0.1, 10.0)
    start_potential = draw_start_potential(jax.random.fold_in(seeds[5], 71), 0)
    cell_feat = draw_cell_feat(jax.random.fold_in(seeds[5], 71), 0)
    site_feat = draw_site_feat(jax.random.fold_in(seeds[5], 71), 0)
    weights = jnp.clip(jnp.exp(jax.random.uniform(seeds[4], (SCEN,), jnp.float32, math.log(0.5), math.log(4.0))), 0.5, 4.0)
    return {"demand": demand, "start_potential": start_potential, "cell_feat": cell_feat, "site_feat": site_feat, "weights": weights}


entropic_eps = 0.25


def tile_costs(cell_cols, site_cols, cell_norm, site_norm):
    inner_prod = jnp.dot(cell_cols.T, site_cols, preferred_element_type=jnp.float32)
    return (cell_norm[:, None] + site_norm[None, :] - 2.0 * inner_prod) / D


def sweep(cell_blocks, norm_blocks, share_blocks, site_cols, site_norm, potential):
    def per_block(carry, block):
        cell_cols, cell_norm, log_share = block
        costs = tile_costs(cell_cols, site_cols, cell_norm, site_norm)
        scores = (potential[None, :] - costs) / entropic_eps
        row_max = jnp.max(scores, axis=1)
        row_lse = row_max + jnp.log(jnp.sum(jnp.exp(scores - row_max[:, None]), axis=1))
        row_pot = entropic_eps * (log_share - row_lse)
        back_scores = (row_pot[:, None] - costs) / entropic_eps
        block_max = jnp.max(back_scores, axis=0)
        block_sum = jnp.sum(jnp.exp(back_scores - block_max[None, :]), axis=0)
        old_max, old_sum = carry
        new_max = jnp.maximum(old_max, block_max)
        new_sum = old_sum * jnp.exp(old_max - new_max) + block_sum * jnp.exp(block_max - new_max)
        return (new_max, new_sum), row_pot

    initial = (jnp.full((SITES,), -jnp.inf, jnp.float32), jnp.zeros((SITES,), jnp.float32))
    (col_max, col_sum), row_pots = lax.scan(per_block, initial, (cell_blocks, norm_blocks, share_blocks))
    return row_pots.reshape(-1), col_max + jnp.log(col_sum)


def reference(demand, start_potential, cell_feat, site_feat, weights):
    cell_wide = cell_feat.astype(jnp.float32)
    cell_norm = jnp.sum(cell_wide * cell_wide, axis=0)
    site_wide = site_feat.astype(jnp.float32)
    site_norm = jnp.sum(site_wide * site_wide, axis=0)
    log_share = jnp.log(demand) - jnp.log(jnp.sum(demand, axis=1, keepdims=True))
    mix_weights = weights / jnp.sum(weights)
    block_count = CELLS // CELL_DEV
    cell_blocks = jnp.transpose(cell_feat.reshape(D, block_count, CELL_DEV), (1, 0, 2))
    norm_blocks = cell_norm.reshape(block_count, CELL_DEV)
    potential = start_potential
    row_pots = jnp.zeros_like(demand)
    log_bary = jnp.zeros((SITES,), jnp.float32)
    for repeat in range(ITERS):
        def per_scenario(inputs):
            share_row, site_row = inputs
            return sweep(cell_blocks, norm_blocks, share_row.reshape(block_count, CELL_DEV), site_feat, site_norm, site_row)

        row_pots, column_lse = lax.map(per_scenario, (log_share, potential))
        log_bary = jnp.sum(mix_weights[:, None] * (potential / entropic_eps + column_lse), axis=0)
        potential = entropic_eps * (log_bary[None, :] - column_lse)
    return row_pots, potential, log_bary
```

```python
import jax
import jax.numpy as jnp
from jax import lax
from jax.experimental import pallas as pl
from jax.experimental.pallas import tpu as pltpu
from jax.sharding import Mesh
from jax.sharding import PartitionSpec as P

ITERS = 2
EPS = 0.25
SCEN = ("z", "y", "core")
CELL_ORDER = ("xh", "z", "y", "core", "xl")
ROW_GROUP = ("xh", "xl", "core")
BARY_GROUP = ("z", "y")
HOME_GROUP = ("xh", "core")
F32 = jnp.float32
BF16 = jnp.bfloat16
SAFE_NORMS = 14400.0
BLK = 256
VMEM = pl.BlockSpec(memory_space=pltpu.VMEM)
SMEM = pl.BlockSpec(memory_space=pltpu.SMEM)


def nt_dot(a, b):
    return lax.dot_general(a, b, (((1,), (1,)), ((), ())), preferred_element_type=F32)


def to_lanes(column):
    n = column.shape[0]
    on = lax.broadcasted_iota(jnp.int32, (n, n), 0) == lax.broadcasted_iota(jnp.int32, (n, n), 1)
    return jnp.sum(jnp.where(on, column, 0.0), axis=0, keepdims=True)


def build_kernel(feat_ref, site_ref, gibbs_ref, rest_ref, cells_ref, sites_ref, site_norm_ref, cell_norm_ref, safe_ref):
    n_cells, width = cells_ref.shape
    n_sites = sites_ref.shape[1]
    depth = site_ref.shape[0]
    per_row = width // depth
    scale = 2.0 / (depth * EPS)
    site = site_ref[...]
    wide = site.astype(F32)
    site_norm = jnp.sum(wide * wide, axis=0, keepdims=True)
    site_norm_ref[...] = site_norm / (depth * EPS)
    spread = (
        lax.broadcasted_iota(jnp.int32, (width, depth), 0) // per_row
        == lax.broadcasted_iota(jnp.int32, (width, depth), 1)
    )
    sites_ref[...] = jnp.dot(
        jnp.where(spread, 1.0, 0.0).astype(BF16), site, preferred_element_type=F32
    ).astype(BF16)
    feat = feat_ref[...]
    rows = lax.broadcasted_iota(jnp.int32, (BLK, width), 0)
    lanes = lax.broadcasted_iota(jnp.int32, (BLK, width), 1)
    own = rows % per_row == lanes % per_row
    ones = jnp.ones((8, width), BF16)

    def cell_block(i, largest):
        at = pl.multiple_of(i * BLK, BLK)
        pick = jnp.where(rows // per_row + i * (BLK // per_row) == lanes, 1.0, 0.0).astype(BF16)
        block = jnp.where(own, jnp.dot(pick, feat, preferred_element_type=F32), 0.0)
        cells_ref[pl.ds(at, BLK), :] = block.astype(BF16)
        square = block * block
        high = square.astype(BF16)
        low = (square - high.astype(F32)).astype(BF16)
        norm = (nt_dot(ones, high) + nt_dot(ones, low))[0:1]
        cell_norm_ref[:, pl.ds(at, BLK)] = norm / (depth * EPS)
        return jnp.maximum(largest, jnp.max(norm))

    largest = lax.fori_loop(0, n_cells // BLK, cell_block, jnp.float32(0.0))
    safe = largest * jnp.max(site_norm) <= SAFE_NORMS
    safe_ref[0, 0] = jnp.where(safe, 1, 0)

    @pl.when(safe)
    def _():
        def tile(t, _):
            i, j = t // (n_sites // 512), t % (n_sites // 512)
            at, to = pl.multiple_of(i * BLK, BLK), pl.multiple_of(j * 512, 512)
            inner = jnp.dot(
                cells_ref[pl.ds(at, BLK), :], sites_ref[:, pl.ds(to, 512)], preferred_element_type=F32
            )
            value = jnp.exp(inner * scale)
            high = value.astype(BF16)
            gibbs_ref[pl.ds(at, BLK), pl.ds(to, 512)] = high
            rest_ref[pl.ds(at, BLK), pl.ds(to, 512)] = (value - high.astype(F32)).astype(BF16)
            return 0

        lax.fori_loop(0, (n_cells // BLK) * (n_sites // 512), tile, 0)


def build(feat, site_feat, quarter, n_sites):
    width = feat.shape[1]
    depth = site_feat.shape[0]
    n_cells = feat.shape[0] * (width // depth)
    return pl.pallas_call(
        build_kernel,
        out_shape=(
            jax.ShapeDtypeStruct((n_cells, n_sites), BF16),
            jax.ShapeDtypeStruct((n_cells, n_sites), BF16),
            jax.ShapeDtypeStruct((n_cells, width), BF16),
            jax.ShapeDtypeStruct((width, n_sites), BF16),
            jax.ShapeDtypeStruct((1, n_sites), F32),
            jax.ShapeDtypeStruct((1, n_cells), F32),
            jax.ShapeDtypeStruct((1, 1), jnp.int32),
        ),
        in_specs=[VMEM, VMEM],
        out_specs=(VMEM, VMEM, VMEM, VMEM, VMEM, VMEM, SMEM),
        compiler_params=pltpu.CompilerParams(vmem_limit_bytes=40 << 20),
        name="build",
    )(feat, lax.dynamic_slice_in_dim(site_feat, quarter * n_sites, n_sites, 1))


def two_parts(factor):
    high = factor.astype(BF16).astype(F32)
    rest = jnp.zeros((4, factor.shape[1]), F32)
    return jnp.concatenate([high, factor - high, rest], axis=0).astype(BF16)


def log_sums(safe, level, gibbs_ref, rest_ref, cells_ref, sites_ref, out_ref, over_sites):
    n_out = out_ref.shape[1]
    scale = 2.0 / ((cells_ref.shape[1] // 8) * EPS)

    @pl.when(safe)
    def _():
        top = jnp.max(level, axis=1, keepdims=True)
        parts = two_parts(jnp.exp(level - top))

        def block(i, _):
            at = pl.multiple_of(i * BLK, BLK)
            if over_sites:
                total = nt_dot(parts, gibbs_ref[pl.ds(at, BLK), :])
                more = nt_dot(parts, rest_ref[pl.ds(at, BLK), :])
            else:
                total = jnp.dot(parts, gibbs_ref[:, pl.ds(at, BLK)], preferred_element_type=F32)
                more = jnp.dot(parts, rest_ref[:, pl.ds(at, BLK)], preferred_element_type=F32)
            out_ref[:, pl.ds(at, BLK)] = top + jnp.log(total[0:2] + (total[2:4] + more[0:2]))
            return 0

        lax.fori_loop(0, n_out // BLK, block, 0)

    @pl.when(jnp.logical_not(safe))
    def _():
        def block(i, _):
            at = pl.multiple_of(i * 128, 128)
            if over_sites:
                inner = jnp.dot(cells_ref[pl.ds(at, 128), :], sites_ref[...], preferred_element_type=F32)
            else:
                inner = lax.dot_general(
                    sites_ref[:, pl.ds(at, 128)],
                    cells_ref[...],
                    (((0,), (1,)), ((), ())),
                    preferred_element_type=F32,
                )
            for s in range(2):
                score = inner * scale + level[s : s + 1]
                top = jnp.max(score, axis=1, keepdims=True)
                total = jnp.sum(jnp.exp(score - top), axis=1, keepdims=True)
                out_ref[s : s + 1, pl.ds(at, 128)] = to_lanes(top + jnp.log(total))
            return 0

        lax.fori_loop(0, n_out // 128, block, 0)


def send_rows(sums_ref, out_ref):
    half = sums_ref.shape[1]
    for s in range(2):
        out_ref[:, s * half : (s + 1) * half] = jnp.broadcast_to(sums_ref[s : s + 1], (out_ref.shape[0], half))


def first_row_kernel(safe_ref, home_ref, site_norm_ref, gibbs_ref, rest_ref, cells_ref, sites_ref, send_ref, level_ref, sums_ref):
    n_demand = home_ref.shape[1] - site_norm_ref.shape[1]
    level = home_ref[0:2, n_demand:] * (1.0 / EPS) - site_norm_ref[...]
    level_ref[...] = level
    log_sums(safe_ref[0, 0] == 1, level, gibbs_ref, rest_ref, cells_ref, sites_ref, sums_ref, True)
    send_rows(sums_ref, send_ref)


def next_row_kernel(safe_ref, terms_ref, column_ref, gibbs_ref, rest_ref, cells_ref, sites_ref, send_ref, level_ref, sums_ref):
    level = jnp.sum(terms_ref[...], axis=0, keepdims=True) - column_ref[...]
    level_ref[...] = level
    log_sums(safe_ref[0, 0] == 1, level, gibbs_ref, rest_ref, cells_ref, sites_ref, sums_ref, True)
    send_rows(sums_ref, send_ref)


def column_kernel(
    safe_ref, pair_ref, weight_ref, home_ref, got_ref, cell_norm_ref, level_ref, gibbs_ref, rest_ref, cells_ref, sites_ref,
    send_ref, column_ref, row_pot_ref,
):
    n_cells = cell_norm_ref.shape[1]
    half = n_cells // 2
    home = home_ref[...]
    demand = jnp.concatenate([home[0:2, :half], home[2:4, :half]], axis=1)
    log_share = jnp.log(demand) - jnp.log(jnp.sum(demand, axis=1, keepdims=True))
    got = got_ref[...]
    top = jnp.max(got, axis=0, keepdims=True)
    row = top + jnp.log(jnp.sum(jnp.exp(got - top), axis=0, keepdims=True))
    down = log_share - jnp.concatenate([row[:, :n_cells], row[:, n_cells:]], axis=0)
    row_pot_ref[...] = EPS * (down + cell_norm_ref[...])
    log_sums(safe_ref[0, 0] == 1, down, gibbs_ref, rest_ref, cells_ref, sites_ref, column_ref, False)
    weight = weight_ref[...]
    which = lax.broadcasted_iota(jnp.int32, weight.shape, 1)
    term = jnp.zeros((1, level_ref.shape[1]), F32)
    for s in range(2):
        own = jnp.sum(jnp.where(which == 2 * pair_ref[0] + s, weight, 0.0), axis=1, keepdims=True)
        term += own / jnp.sum(weight, axis=1, keepdims=True) * (level_ref[s : s + 1] + column_ref[s : s + 1])
    send_ref[...] = jnp.broadcast_to(term, send_ref.shape)


def last_kernel(terms_ref, column_ref, site_norm_ref, send_ref):
    n_sites = site_norm_ref.shape[1]
    log_bary = jnp.sum(terms_ref[...], axis=0, keepdims=True)
    potential = EPS * (log_bary - column_ref[...] + site_norm_ref[...])
    send_ref[:, :n_sites] = jnp.concatenate([potential, potential], axis=0)
    send_ref[:, n_sites:] = jnp.broadcast_to(log_bary, (4, n_sites))


def call(kernel, outs, *args, scratch=()):
    return pl.pallas_call(
        kernel,
        out_shape=tuple(jax.ShapeDtypeStruct(s, F32) for s in outs),
        in_specs=[SMEM if a.dtype == jnp.int32 else VMEM for a in args],
        out_specs=(VMEM,) * len(outs),
        scratch_shapes=[pltpu.VMEM(s, F32) for s in scratch],
        compiler_params=pltpu.CompilerParams(vmem_limit_bytes=40 << 20),
        name=kernel.__name__,
    )(*args)


def exchange(value, axes):
    return lax.all_to_all(value, axes, split_axis=0, concat_axis=0, tiled=True)


def on_device(demand, start_potential, cell_feat, site_feat, weights):
    n_home = lax.axis_size(HOME_GROUP)
    n_row = lax.axis_size(ROW_GROUP)
    n_bary = lax.axis_size(BARY_GROUP)
    n_sites = start_potential.shape[1] // n_home
    n_cells = demand.shape[1] * 2
    quarter = lax.axis_index(HOME_GROUP)
    pair = lax.axis_index(BARY_GROUP).astype(jnp.int32).reshape(1)
    core, xh = lax.axis_index("core"), lax.axis_index("xh")

    packed = cell_feat.reshape(1, -1)
    feat = exchange(jnp.broadcast_to(packed, (lax.axis_size(CELL_ORDER), packed.shape[1])), CELL_ORDER)
    home = exchange(
        jnp.concatenate(
            [jnp.broadcast_to(demand, (n_home, demand.shape[1])), start_potential.reshape(n_home, n_sites)], axis=1
        ),
        HOME_GROUP,
    )
    gibbs, rest, cells, sites, site_norm, cell_norm, safe = build(feat, site_feat, quarter, n_sites)
    weight = weights.reshape(1, -1)
    sums = [(2, n_cells)]
    send, level = call(
        first_row_kernel, [(n_row, 2 * n_cells), (2, n_sites)], safe, home, site_norm, gibbs, rest, cells, sites, scratch=sums
    )
    for repeat in range(ITERS):
        got = exchange(send, ROW_GROUP)
        send, column, row_pot = call(
            column_kernel, [(n_bary, n_sites), (2, n_sites), (2, n_cells)],
            safe, pair, weight, home, got, cell_norm, level, gibbs, rest, cells, sites,
        )
        terms = exchange(send, BARY_GROUP)
        if repeat < ITERS - 1:
            send, level = call(
                next_row_kernel, [(n_row, 2 * n_cells), (2, n_sites)], safe, terms, column, gibbs, rest, cells, sites, scratch=sums
            )
    (send,) = call(last_kernel, [(n_home, 2 * n_sites)], terms, column, site_norm)
    both = exchange(send, HOME_GROUP)
    own_pot = lax.dynamic_slice(row_pot, (core, xh * demand.shape[1]), demand.shape)
    return own_pot, both[:, :n_sites].reshape(1, -1), both[:, n_sites:].reshape(-1)


def solution(mesh):
    torus = Mesh(
        mesh.devices.reshape(8, 4, 2, mesh.shape["cell"], mesh.shape["site"]), ("z", "y", "core", "xh", "xl")
    )
    return jax.shard_map(
        on_device,
        mesh=torus,
        in_specs=(P(SCEN, "xh"), P(SCEN, "xl"), P(None, CELL_ORDER), P(None, "xl"), P()),
        out_specs=(P(SCEN, "xh"), P(SCEN, "xl"), P("xl")),
        check_vma=False,
    )
```

```python
import math

import jax
import jax.numpy as jnp
from jax import lax
from jax.experimental import pallas as pl
from jax.experimental.pallas import tpu as pltpu
from jax.sharding import Mesh
from jax.sharding import PartitionSpec as P

ITERS = 2
EPS = 0.25
SCEN = ("z", "y", "core")
CELL_ORDER = ("xh", "z", "y", "core", "xl")
ROW_GROUP = ("xh", "xl", "core")
BARY_GROUP = ("z", "y")
HOME_GROUP = ("xh", "core")
F32 = jnp.float32
BF16 = jnp.bfloat16
SAFE_NORMS = 14400.0
LANE = 128
VMEM = pl.BlockSpec(memory_space=pltpu.VMEM)
SMEM = pl.BlockSpec(memory_space=pltpu.SMEM)


def nt_dot(a, b):
    return lax.dot_general(a, b, (((1,), (1,)), ((), ())), preferred_element_type=F32)


def diagonal():
    shape = (LANE, LANE)
    return lax.broadcasted_iota(jnp.int32, shape, 0) == lax.broadcasted_iota(jnp.int32, shape, 1)


def to_row(column):
    return jnp.sum(jnp.where(diagonal(), column, 0.0), axis=0, keepdims=True)


def to_column(row):
    return jnp.sum(jnp.where(diagonal(), row, 0.0), axis=1, keepdims=True)


def block_at(i, size):
    return pl.ds(pl.multiple_of(i * size, size), size)


def call(kernel, outs, *args, scratch=(), limit=16):
    def spec(a):
        return SMEM if a.dtype == jnp.int32 else VMEM

    outs = tuple(jax.ShapeDtypeStruct(*o) for o in outs)
    return pl.pallas_call(
        kernel,
        out_shape=outs,
        in_specs=[spec(a) for a in args],
        out_specs=tuple(spec(o) for o in outs),
        scratch_shapes=[pltpu.VMEM(s, F32) for s in scratch],
        compiler_params=pltpu.CompilerParams(vmem_limit_bytes=limit << 20),
        name=kernel.__name__,
    )(*args)


def pack_kernel(feat_ref, out_ref):
    depth, per_row = feat_ref.shape
    width = depth * per_row
    spread = lax.broadcasted_iota(jnp.int32, (per_row, width), 1) % per_row == lax.broadcasted_iota(
        jnp.int32, (per_row, width), 0
    )
    wide = jnp.dot(feat_ref[...], jnp.where(spread, 1.0, 0.0).astype(BF16), preferred_element_type=F32)
    own = lax.broadcasted_iota(jnp.int32, (depth, width), 1) // per_row == lax.broadcasted_iota(
        jnp.int32, (depth, width), 0
    )
    line = jnp.sum(jnp.where(own, wide, 0.0), axis=0, keepdims=True)
    lines = jnp.concatenate([line[:, h * LANE : (h + 1) * LANE] for h in range(width // LANE)], axis=0)
    out_ref[...] = jnp.broadcast_to(lines.astype(BF16)[None], out_ref.shape)


def build_kernel(feat_ref, site_ref, gibbs_ref, cells_ref, sites_ref, site_norm_ref, cell_norm_ref, safe_ref):
    n_cells, width = cells_ref.shape
    n_sites = sites_ref.shape[1]
    depth = site_ref.shape[0]
    per_row = width // depth
    rows_blk, cols_blk = 256, 512
    site = site_ref[...]
    wide = site.astype(F32)
    site_norm = jnp.sum(wide * wide, axis=0, keepdims=True)
    for b in range(n_sites // LANE):
        site_norm_ref[b : b + 1, :] = site_norm[:, b * LANE : (b + 1) * LANE] / (depth * EPS)
    spread = (
        lax.broadcasted_iota(jnp.int32, (width, depth), 0) // per_row
        == lax.broadcasted_iota(jnp.int32, (width, depth), 1)
    )
    sites_ref[...] = jnp.dot(
        jnp.where(spread, 1.0, 0.0).astype(BF16), site, preferred_element_type=F32
    ).astype(BF16)
    feat = feat_ref[...]
    rows = lax.broadcasted_iota(jnp.int32, (rows_blk, width), 0)
    lanes = lax.broadcasted_iota(jnp.int32, (rows_blk, width), 1)
    own = rows % per_row == lanes % per_row
    ones = jnp.ones((8, width), BF16)
    largest = jnp.float32(0.0)
    for i in range(n_cells // rows_blk):
        pick = jnp.where(rows // per_row + i * (rows_blk // per_row) == lanes, 1.0, 0.0).astype(BF16)
        block = jnp.where(own, jnp.dot(pick, feat, preferred_element_type=F32), 0.0)
        cells_ref[i * rows_blk : (i + 1) * rows_blk, :] = block.astype(BF16)
        square = block * block
        high = square.astype(BF16)
        low = (square - high.astype(F32)).astype(BF16)
        norm = (nt_dot(ones, high) + nt_dot(ones, low))[0:1]
        for b in range(rows_blk // LANE):
            at = i * (rows_blk // LANE) + b
            cell_norm_ref[at : at + 1, :] = norm[:, b * LANE : (b + 1) * LANE] / (depth * EPS)
        largest = jnp.maximum(largest, jnp.max(norm))
    safe = largest * jnp.max(site_norm) <= SAFE_NORMS
    safe_ref[0, 0] = jnp.where(safe, 1, 0)

    @pl.when(safe)
    def _():
        scale = 2.0 / (depth * EPS) * math.log2(math.e)

        def tile(t, _):
            at = block_at(t // (n_sites // cols_blk), rows_blk)
            to = block_at(t % (n_sites // cols_blk), cols_blk)
            inner = jnp.dot(cells_ref[at, :], sites_ref[:, to], preferred_element_type=F32)
            gibbs_ref[at, to] = jnp.exp2(inner * scale)
            return 0

        lax.fori_loop(0, (n_cells // rows_blk) * (n_sites // cols_blk), tile, 0)


def log_sums(safe, level, gibbs_ref, cells_ref, sites_ref, out_ref, part_ref, sum_ref, over_sites):
    n_scen, blocks_in, _ = level.shape
    blocks_out = out_ref.shape[1]
    scale = 2.0 / ((cells_ref.shape[1] // 8) * EPS)

    @pl.when(safe)
    def _():
        top = jnp.max(jnp.max(level, axis=2, keepdims=True), axis=1, keepdims=True)
        part_ref[...] = jnp.exp(level - top)
        if over_sites:

            def cell_block(i, _):
                at = block_at(i, LANE)
                sums = [jnp.zeros((LANE, LANE), F32) for _ in range(n_scen)]
                for b in range(blocks_in):
                    tile = gibbs_ref[at, b * LANE : (b + 1) * LANE]
                    for s in range(n_scen):
                        sums[s] += tile * part_ref[s, b : b + 1, :]
                for s in range(n_scen):
                    out_ref[s, pl.ds(i, 1), :] = to_row(jnp.sum(sums[s], axis=1, keepdims=True))
                return 0

            lax.fori_loop(0, blocks_out, cell_block, 0)
        else:
            sum_ref[...] = jnp.zeros_like(sum_ref)

            def cell_block(i, _):
                at = block_at(i, LANE)
                columns = [
                    jnp.broadcast_to(to_column(part_ref[s, pl.ds(i, 1), :]), (LANE, LANE)) for s in range(n_scen)
                ]
                for b in range(blocks_out):
                    tile = gibbs_ref[at, b * LANE : (b + 1) * LANE]
                    for s in range(n_scen):
                        sum_ref[s, b] += jnp.sum((tile * columns[s]).reshape(LANE // 8, 8, LANE), axis=0)
                return 0

            lax.fori_loop(0, blocks_in, cell_block, 0)
            out_ref[...] = jnp.sum(sum_ref[...], axis=2)
        out_ref[...] = top + jnp.log(out_ref[...])

    @pl.when(jnp.logical_not(safe))
    def _():
        def block(i, _):
            at = block_at(i, LANE)
            if over_sites:
                inner = jnp.dot(cells_ref[at, :], sites_ref[...], preferred_element_type=F32)
            else:
                inner = lax.dot_general(
                    sites_ref[:, at], cells_ref[...], (((0,), (1,)), ((), ())), preferred_element_type=F32
                )
            for s in range(n_scen):
                score = inner * scale + jnp.concatenate([level[s, b : b + 1, :] for b in range(blocks_in)], axis=1)
                top = jnp.max(score, axis=1, keepdims=True)
                total = jnp.sum(jnp.exp(score - top), axis=1, keepdims=True)
                out_ref[s, pl.ds(i, 1), :] = to_row(top + jnp.log(total))
            return 0

        lax.fori_loop(0, blocks_out, block, 0)


def first_row_kernel(
    safe_ref, home_ref, site_norm_ref, gibbs_ref, cells_ref, sites_ref, send_ref, level_ref, out_ref, part_ref
):
    n_blocks = site_norm_ref.shape[0]
    level = home_ref[0:2, home_ref.shape[1] - n_blocks :, :] * (1.0 / EPS) - site_norm_ref[...][None]
    level_ref[...] = level
    log_sums(safe_ref[0, 0] == 1, level, gibbs_ref, cells_ref, sites_ref, out_ref, part_ref, None, True)
    send_ref[...] = jnp.broadcast_to(out_ref[...][None], send_ref.shape)


def next_row_kernel(
    safe_ref, terms_ref, column_ref, gibbs_ref, cells_ref, sites_ref, send_ref, level_ref, out_ref, part_ref
):
    level = jnp.sum(terms_ref[...], axis=0)[None] - column_ref[...]
    level_ref[...] = level
    log_sums(safe_ref[0, 0] == 1, level, gibbs_ref, cells_ref, sites_ref, out_ref, part_ref, None, True)
    send_ref[...] = jnp.broadcast_to(out_ref[...][None], send_ref.shape)


def column_kernel(
    safe_ref, place_ref, weight_ref, home_ref, got_ref, cell_norm_ref, level_ref, gibbs_ref, cells_ref, sites_ref,
    send_ref, column_ref, row_pot_ref, part_ref, sum_ref,
):
    half = row_pot_ref.shape[0]
    home = home_ref[...]
    demand = jnp.concatenate([home[0:2, :half], home[2:4, :half]], axis=1)
    total = jnp.sum(jnp.sum(demand, axis=2, keepdims=True), axis=1, keepdims=True)
    got = got_ref[...]
    top = jnp.max(got, axis=0)
    row = top + jnp.log(jnp.sum(jnp.exp(got - top[None]), axis=0))
    down = jnp.log(demand) - jnp.log(total) - row
    own = jnp.where(place_ref[1] == 0, down[0], down[1])
    norm = cell_norm_ref[...]
    first = place_ref[2] == 0
    row_pot_ref[...] = EPS * (jnp.where(first, own[:half], own[half:]) + jnp.where(first, norm[:half], norm[half:]))
    log_sums(safe_ref[0, 0] == 1, down, gibbs_ref, cells_ref, sites_ref, column_ref, part_ref, sum_ref, False)
    weight = weight_ref[...]
    which = lax.broadcasted_iota(jnp.int32, weight.shape, 1)
    term = jnp.zeros(level_ref.shape[1:], F32)
    for s in range(2):
        own_weight = jnp.sum(jnp.where(which == 2 * place_ref[0] + s, weight, 0.0), axis=1, keepdims=True)
        term += own_weight / jnp.sum(weight, axis=1, keepdims=True) * (level_ref[s] + column_ref[s])
    send_ref[...] = jnp.broadcast_to(term[None], send_ref.shape)


def last_kernel(terms_ref, column_ref, site_norm_ref, send_ref):
    n_blocks = site_norm_ref.shape[0]
    log_bary = jnp.sum(terms_ref[...], axis=0)
    potential = EPS * (log_bary[None] - column_ref[...] + site_norm_ref[...][None])
    send_ref[:, :n_blocks, :] = jnp.concatenate([potential, potential], axis=0)
    send_ref[:, n_blocks:, :] = jnp.broadcast_to(log_bary[None], (4, n_blocks, LANE))


def exchange(value, axes):
    return lax.all_to_all(value, axes, split_axis=0, concat_axis=0, tiled=True)


def on_device(demand, start_potential, cell_feat, site_feat, weights):
    n_home = lax.axis_size(HOME_GROUP)
    n_row = lax.axis_size(ROW_GROUP)
    n_bary = lax.axis_size(BARY_GROUP)
    n_sites = start_potential.shape[1] // n_home
    n_cells = demand.shape[1] * 2
    site_blocks, cell_blocks = n_sites // LANE, n_cells // LANE
    quarter = lax.axis_index(HOME_GROUP)
    place = jnp.stack([lax.axis_index(BARY_GROUP), lax.axis_index("core"), lax.axis_index("xh")]).astype(jnp.int32)

    width = cell_feat.size
    n_all = lax.axis_size(CELL_ORDER)
    (packed,) = call(pack_kernel, [((n_all, width // LANE, LANE), BF16)], cell_feat)
    packed, demand, start_potential = lax.optimization_barrier((packed, demand, start_potential))
    feat = exchange(packed, CELL_ORDER).reshape(n_all, width)
    shares = jnp.broadcast_to(demand.reshape(1, -1, LANE), (n_home, cell_blocks // 2, LANE))
    home = exchange(
        jnp.concatenate([shares, start_potential.reshape(n_home, site_blocks, LANE)], axis=1), HOME_GROUP
    )
    own_sites = lax.dynamic_slice_in_dim(site_feat, quarter * n_sites, n_sites, 1)
    weight = weights.reshape(1, -1)
    feat, home, own_sites, place, weight = lax.optimization_barrier((feat, home, own_sites, place, weight))
    gibbs, cells, sites, site_norm, cell_norm, safe = call(
        build_kernel,
        [
            ((n_cells, n_sites), F32),
            ((n_cells, width), BF16),
            ((width, n_sites), BF16),
            ((site_blocks, LANE), F32),
            ((cell_blocks, LANE), F32),
            ((1, 1), jnp.int32),
        ],
        feat, own_sites, limit=24,
    )
    on_cells, on_sites = (2, cell_blocks, LANE), (2, site_blocks, LANE)
    row_outs = [((n_row, *on_cells), F32), (on_sites, F32)]
    row_scratch = [on_cells, on_sites]
    send, level = call(
        first_row_kernel, row_outs, safe, home, site_norm, gibbs, cells, sites, scratch=row_scratch
    )
    for repeat in range(ITERS):
        got = exchange(send, ROW_GROUP)
        send, column, row_pot = call(
            column_kernel,
            [((n_bary, site_blocks, LANE), F32), (on_sites, F32), ((cell_blocks // 2, LANE), F32)],
            safe, place, weight, home, got, cell_norm, level, gibbs, cells, sites,
            scratch=[on_cells, (2, site_blocks, 8, LANE)],
        )
        terms = exchange(send, BARY_GROUP)
        if repeat < ITERS - 1:
            send, level = call(
                next_row_kernel, row_outs, safe, terms, column, gibbs, cells, sites, scratch=row_scratch
            )
    (send,) = call(last_kernel, [((n_home, 2 * site_blocks, LANE), F32)], terms, column, site_norm)
    both = exchange(send, HOME_GROUP)
    return row_pot.reshape(1, -1), both[:, :site_blocks].reshape(1, -1), both[:, site_blocks:].reshape(-1)


def solution(mesh):
    torus = Mesh(
        mesh.devices.reshape(8, 4, 2, mesh.shape["cell"], mesh.shape["site"]), ("z", "y", "core", "xh", "xl")
    )
    return jax.shard_map(
        on_device,
        mesh=torus,
        in_specs=(P(SCEN, "xh"), P(SCEN, "xl"), P(None, CELL_ORDER), P(None, "xl"), P()),
        out_specs=(P(SCEN, "xh"), P(SCEN, "xl"), P("xl")),
        check_vma=False,
    )
```

```python
import math

import jax
import jax.numpy as jnp
from jax import lax
from jax.experimental import pallas as pl
from jax.experimental.pallas import tpu as pltpu
from jax.sharding import Mesh
from jax.sharding import PartitionSpec as P

ITERS = 2
EPS = 0.25
SCEN = ("z", "y", "core")
CELL_ORDER = ("xh", "z", "y", "core", "xl")
ROW_GROUP = ("xh", "xl", "core")
BARY_GROUP = ("z", "y")
HOME_GROUP = ("xh", "core")
F32 = jnp.float32
BF16 = jnp.bfloat16
SAFE_NORMS = 14400.0
LANE = 128
VMEM = pl.BlockSpec(memory_space=pltpu.VMEM)
SMEM = pl.BlockSpec(memory_space=pltpu.SMEM)


def nt_dot(a, b):
    return lax.dot_general(a, b, (((1,), (1,)), ((), ())), preferred_element_type=F32)


def diagonal():
    shape = (LANE, LANE)
    return lax.broadcasted_iota(jnp.int32, shape, 0) == lax.broadcasted_iota(jnp.int32, shape, 1)


def to_row(column):
    return jnp.sum(jnp.where(diagonal(), column, 0.0), axis=0, keepdims=True)


def to_column(row):
    return jnp.sum(jnp.where(diagonal(), row, 0.0), axis=1, keepdims=True)


def block_at(i, size):
    return pl.ds(pl.multiple_of(i * size, size), size)


def unrolled_loop(steps, by, body):
    def several(i, _):
        for u in range(by):
            body(i * by + u)
        return 0

    lax.fori_loop(0, steps // by, several, 0)


def call(kernel, outs, *args, scratch=(), limit=16):
    def spec(a):
        return SMEM if a.dtype == jnp.int32 else VMEM

    outs = tuple(jax.ShapeDtypeStruct(*o) for o in outs)
    return pl.pallas_call(
        kernel,
        out_shape=outs,
        in_specs=[spec(a) for a in args],
        out_specs=tuple(spec(o) for o in outs),
        scratch_shapes=[pltpu.VMEM(s, F32) for s in scratch],
        compiler_params=pltpu.CompilerParams(vmem_limit_bytes=limit << 20),
        name=kernel.__name__,
    )(*args)


def pack_kernel(feat_ref, out_ref):
    depth, per_row = feat_ref.shape
    width = depth * per_row
    spread = lax.broadcasted_iota(jnp.int32, (per_row, width), 1) % per_row == lax.broadcasted_iota(
        jnp.int32, (per_row, width), 0
    )
    wide = jnp.dot(feat_ref[...], jnp.where(spread, 1.0, 0.0).astype(BF16), preferred_element_type=F32)
    own = lax.broadcasted_iota(jnp.int32, (depth, width), 1) // per_row == lax.broadcasted_iota(
        jnp.int32, (depth, width), 0
    )
    line = jnp.sum(jnp.where(own, wide, 0.0), axis=0, keepdims=True)
    lines = jnp.concatenate([line[:, h * LANE : (h + 1) * LANE] for h in range(width // LANE)], axis=0)
    out_ref[...] = jnp.broadcast_to(lines.astype(BF16)[None], out_ref.shape)


def build_kernel(feat_ref, site_ref, gibbs_ref, cells_ref, sites_ref, site_norm_ref, cell_norm_ref, safe_ref):
    n_cells, width = cells_ref.shape
    n_sites = sites_ref.shape[1]
    depth = site_ref.shape[0]
    per_row = width // depth
    rows_blk, cols_blk = 256, 512
    site = site_ref[...]
    wide = site.astype(F32)
    site_norm = jnp.sum(wide * wide, axis=0, keepdims=True)
    for b in range(n_sites // LANE):
        site_norm_ref[b : b + 1, :] = site_norm[:, b * LANE : (b + 1) * LANE] / (depth * EPS)
    spread = (
        lax.broadcasted_iota(jnp.int32, (width, depth), 0) // per_row
        == lax.broadcasted_iota(jnp.int32, (width, depth), 1)
    )
    sites_ref[...] = jnp.dot(
        jnp.where(spread, 1.0, 0.0).astype(BF16), site, preferred_element_type=F32
    ).astype(BF16)
    feat = feat_ref[...]
    rows = lax.broadcasted_iota(jnp.int32, (rows_blk, width), 0)
    lanes = lax.broadcasted_iota(jnp.int32, (rows_blk, width), 1)
    own = rows % per_row == lanes % per_row
    ones = jnp.ones((8, width), BF16)
    largest = jnp.float32(0.0)
    for i in range(n_cells // rows_blk):
        pick = jnp.where(rows // per_row + i * (rows_blk // per_row) == lanes, 1.0, 0.0).astype(BF16)
        block = jnp.where(own, jnp.dot(pick, feat, preferred_element_type=F32), 0.0)
        cells_ref[i * rows_blk : (i + 1) * rows_blk, :] = block.astype(BF16)
        square = block * block
        high = square.astype(BF16)
        low = (square - high.astype(F32)).astype(BF16)
        norm = (nt_dot(ones, high) + nt_dot(ones, low))[0:1]
        for b in range(rows_blk // LANE):
            at = i * (rows_blk // LANE) + b
            cell_norm_ref[at : at + 1, :] = norm[:, b * LANE : (b + 1) * LANE] / (depth * EPS)
        largest = jnp.maximum(largest, jnp.max(norm))
    safe = largest * jnp.max(site_norm) <= SAFE_NORMS
    safe_ref[0, 0] = jnp.where(safe, 1, 0)

    @pl.when(safe)
    def _():
        scale = 2.0 / (depth * EPS) * math.log2(math.e)

        def tile(t):
            at = block_at(t // (n_sites // cols_blk), rows_blk)
            to = block_at(t % (n_sites // cols_blk), cols_blk)
            inner = jnp.dot(cells_ref[at, :], sites_ref[:, to], preferred_element_type=F32)
            gibbs_ref[at, to] = jnp.exp2(inner * scale)

        unrolled_loop((n_cells // rows_blk) * (n_sites // cols_blk), 4, tile)


def log_sums(safe, level, gibbs_ref, cells_ref, sites_ref, out_ref, part_ref, sum_ref, over_sites):
    n_scen, blocks_in, _ = level.shape
    blocks_out = out_ref.shape[1]
    scale = 2.0 / ((cells_ref.shape[1] // 8) * EPS)

    @pl.when(safe)
    def _():
        top = jnp.max(jnp.max(level, axis=2, keepdims=True), axis=1, keepdims=True)
        part_ref[...] = jnp.exp(level - top)
        if over_sites:

            def cell_block(i):
                at = block_at(i, LANE)
                sums = [jnp.zeros((LANE, LANE), F32) for _ in range(n_scen)]
                for b in range(blocks_in):
                    tile = gibbs_ref[at, b * LANE : (b + 1) * LANE]
                    for s in range(n_scen):
                        sums[s] += tile * part_ref[s, b : b + 1, :]
                for s in range(n_scen):
                    out_ref[s, pl.ds(i, 1), :] = to_row(jnp.sum(sums[s], axis=1, keepdims=True))

            unrolled_loop(blocks_out, 4, cell_block)
        else:
            sum_ref[...] = jnp.zeros_like(sum_ref)

            def cell_block(i):
                at = block_at(i, LANE)
                columns = [
                    jnp.broadcast_to(to_column(part_ref[s, pl.ds(i, 1), :]), (LANE, LANE)) for s in range(n_scen)
                ]
                for b in range(blocks_out):
                    tile = gibbs_ref[at, b * LANE : (b + 1) * LANE]
                    for s in range(n_scen):
                        sum_ref[s, b] += jnp.sum((tile * columns[s]).reshape(LANE // 8, 8, LANE), axis=0)

            unrolled_loop(blocks_in, 4, cell_block)
            out_ref[...] = jnp.sum(sum_ref[...], axis=2)
        out_ref[...] = top + jnp.log(out_ref[...])

    @pl.when(jnp.logical_not(safe))
    def _():
        def block(i, _):
            at = block_at(i, LANE)
            if over_sites:
                inner = jnp.dot(cells_ref[at, :], sites_ref[...], preferred_element_type=F32)
            else:
                inner = lax.dot_general(
                    sites_ref[:, at], cells_ref[...], (((0,), (1,)), ((), ())), preferred_element_type=F32
                )
            for s in range(n_scen):
                score = inner * scale + jnp.concatenate([level[s, b : b + 1, :] for b in range(blocks_in)], axis=1)
                top = jnp.max(score, axis=1, keepdims=True)
                total = jnp.sum(jnp.exp(score - top), axis=1, keepdims=True)
                out_ref[s, pl.ds(i, 1), :] = to_row(top + jnp.log(total))
            return 0

        lax.fori_loop(0, blocks_out, block, 0)


def first_row_kernel(
    safe_ref, pots_ref, site_norm_ref, gibbs_ref, cells_ref, sites_ref, send_ref, level_ref, out_ref, part_ref
):
    level = pots_ref[...] * (1.0 / EPS) - site_norm_ref[...][None]
    level_ref[...] = level
    log_sums(safe_ref[0, 0] == 1, level, gibbs_ref, cells_ref, sites_ref, out_ref, part_ref, None, True)
    send_ref[...] = jnp.broadcast_to(out_ref[...][None], send_ref.shape)


def next_row_kernel(
    safe_ref, terms_ref, column_ref, gibbs_ref, cells_ref, sites_ref, send_ref, level_ref, out_ref, part_ref
):
    level = jnp.sum(terms_ref[...], axis=0)[None] - column_ref[...]
    level_ref[...] = level
    log_sums(safe_ref[0, 0] == 1, level, gibbs_ref, cells_ref, sites_ref, out_ref, part_ref, None, True)
    send_ref[...] = jnp.broadcast_to(out_ref[...][None], send_ref.shape)


def column_kernel(
    safe_ref, place_ref, weight_ref, shares_ref, got_ref, cell_norm_ref, level_ref, gibbs_ref, cells_ref, sites_ref,
    send_ref, column_ref, row_pot_ref, part_ref, sum_ref,
):
    half = row_pot_ref.shape[0]
    demand = shares_ref[...]
    total = jnp.sum(jnp.sum(demand, axis=2, keepdims=True), axis=1, keepdims=True)
    got = got_ref[...]
    top = jnp.max(got, axis=0)
    row = top + jnp.log(jnp.sum(jnp.exp(got - top[None]), axis=0))
    down = jnp.log(demand) - jnp.log(total) - row
    own = jnp.where(place_ref[1] == 0, down[0], down[1])
    norm = cell_norm_ref[...]
    first = place_ref[2] == 0
    row_pot_ref[...] = EPS * (jnp.where(first, own[:half], own[half:]) + jnp.where(first, norm[:half], norm[half:]))
    log_sums(safe_ref[0, 0] == 1, down, gibbs_ref, cells_ref, sites_ref, column_ref, part_ref, sum_ref, False)
    weight = weight_ref[...]
    which = lax.broadcasted_iota(jnp.int32, weight.shape, 1)
    term = jnp.zeros(level_ref.shape[1:], F32)
    for s in range(2):
        own_weight = jnp.sum(jnp.where(which == 2 * place_ref[0] + s, weight, 0.0), axis=1, keepdims=True)
        term += own_weight / jnp.sum(weight, axis=1, keepdims=True) * (level_ref[s] + column_ref[s])
    send_ref[...] = jnp.broadcast_to(term[None], send_ref.shape)


def last_kernel(terms_ref, column_ref, site_norm_ref, send_ref):
    n_blocks = site_norm_ref.shape[0]
    log_bary = jnp.sum(terms_ref[...], axis=0)
    potential = EPS * (log_bary[None] - column_ref[...] + site_norm_ref[...][None])
    send_ref[:, :n_blocks, :] = jnp.concatenate([potential, potential], axis=0)
    send_ref[:, n_blocks:, :] = jnp.broadcast_to(log_bary[None], (4, n_blocks, LANE))


def exchange(value, axes):
    return lax.all_to_all(value, axes, split_axis=0, concat_axis=0, tiled=True)


def swapped(value, axis):
    return lax.ppermute(value, axis, [(0, 1), (1, 0)])


def on_device(demand, start_potential, cell_feat, site_feat, weights):
    n_home = lax.axis_size(HOME_GROUP)
    n_row = lax.axis_size(ROW_GROUP)
    n_bary = lax.axis_size(BARY_GROUP)
    n_sites = start_potential.shape[1] // n_home
    n_cells = demand.shape[1] * 2
    site_blocks, cell_blocks = n_sites // LANE, n_cells // LANE
    quarter = lax.axis_index(HOME_GROUP)
    place = jnp.stack([lax.axis_index(BARY_GROUP), lax.axis_index("core"), lax.axis_index("xh")]).astype(jnp.int32)

    width = cell_feat.size
    n_all = lax.axis_size(CELL_ORDER)
    (packed,) = call(pack_kernel, [((n_all, width // LANE, LANE), BF16)], cell_feat)
    packed, demand, start_potential = lax.optimization_barrier((packed, demand, start_potential))
    feat = exchange(packed, CELL_ORDER).reshape(n_all, width)
    core, far = lax.axis_index("core"), lax.axis_index("xh")
    pots = start_potential.reshape(2, 2, site_blocks, LANE)
    pots = jnp.where(far == 0, pots[0], pots[1])
    share = demand.reshape(-1, LANE)
    from_core = swapped(jnp.concatenate([share, jnp.where(core == 0, pots[1], pots[0])], axis=0), "core")
    other_share, other_pot = from_core[: cell_blocks // 2], from_core[cell_blocks // 2 :]
    own_pot = jnp.where(core == 0, pots[0], pots[1])
    pots = jnp.where(core == 0, jnp.stack([own_pot, other_pot]), jnp.stack([other_pot, own_pot]))
    shares = jnp.where(core == 0, jnp.stack([share, other_share]), jnp.stack([other_share, share]))
    far_shares = swapped(shares, "xh")
    shares = jnp.where(
        far == 0, jnp.concatenate([shares, far_shares], axis=1), jnp.concatenate([far_shares, shares], axis=1)
    )
    own_sites = lax.dynamic_slice_in_dim(site_feat, quarter * n_sites, n_sites, 1)
    weight = weights.reshape(1, -1)
    feat, pots, shares, own_sites, place, weight = lax.optimization_barrier((feat, pots, shares, own_sites, place, weight))
    gibbs, cells, sites, site_norm, cell_norm, safe = call(
        build_kernel,
        [
            ((n_cells, n_sites), F32),
            ((n_cells, width), BF16),
            ((width, n_sites), BF16),
            ((site_blocks, LANE), F32),
            ((cell_blocks, LANE), F32),
            ((1, 1), jnp.int32),
        ],
        feat, own_sites, limit=24,
    )
    on_cells, on_sites = (2, cell_blocks, LANE), (2, site_blocks, LANE)
    row_outs = [((n_row, *on_cells), F32), (on_sites, F32)]
    row_scratch = [on_cells, on_sites]
    send, level = call(
        first_row_kernel, row_outs, safe, pots, site_norm, gibbs, cells, sites, scratch=row_scratch
    )
    for repeat in range(ITERS):
        got = exchange(send, ROW_GROUP)
        send, column, row_pot = call(
            column_kernel,
            [((n_bary, site_blocks, LANE), F32), (on_sites, F32), ((cell_blocks // 2, LANE), F32)],
            safe, place, weight, shares, got, cell_norm, level, gibbs, cells, sites,
            scratch=[on_cells, (2, site_blocks, 8, LANE)],
        )
        terms = exchange(send, BARY_GROUP)
        if repeat < ITERS - 1:
            send, level = call(
                next_row_kernel, row_outs, safe, terms, column, gibbs, cells, sites, scratch=row_scratch
            )
    (send,) = call(last_kernel, [((n_home, 2 * site_blocks, LANE), F32)], terms, column, site_norm)
    both = exchange(send, HOME_GROUP)
    return row_pot.reshape(1, -1), both[:, :site_blocks].reshape(1, -1), both[:, site_blocks:].reshape(-1)


def solution(mesh):
    torus = Mesh(
        mesh.devices.reshape(8, 4, 2, mesh.shape["cell"], mesh.shape["site"]), ("z", "y", "core", "xh", "xl")
    )
    return jax.shard_map(
        on_device,
        mesh=torus,
        in_specs=(P(SCEN, "xh"), P(SCEN, "xl"), P(None, CELL_ORDER), P(None, "xl"), P()),
        out_specs=(P(SCEN, "xh"), P(SCEN, "xl"), P("xl")),
        check_vma=False,
    )
```

```python
import math

import jax
import jax.numpy as jnp
from jax import lax
from jax.experimental import pallas as pl
from jax.experimental.pallas import tpu as pltpu
from jax.sharding import Mesh
from jax.sharding import PartitionSpec as P

ITERS = 2
EPS = 0.25
SCEN = ("z", "y", "core")
CELL_ORDER = ("xh", "z", "y", "core", "xl")
ROW_GROUP = ("xh", "xl", "core")
BARY_GROUP = ("z", "y")
HOME_GROUP = ("xh", "core")
SWAP_GROUP = ("core", "xh")
CORE, FAR, CROSS = 2, 1, 3
F32 = jnp.float32
BF16 = jnp.bfloat16
SAFE_NORMS = 14400.0
LANE = 128
VMEM = pl.BlockSpec(memory_space=pltpu.VMEM)
SMEM = pl.BlockSpec(memory_space=pltpu.SMEM)


def diagonal():
    shape = (LANE, LANE)
    return lax.broadcasted_iota(jnp.int32, shape, 0) == lax.broadcasted_iota(jnp.int32, shape, 1)


def to_row(column):
    return jnp.sum(jnp.where(diagonal(), column, 0.0), axis=0, keepdims=True)


def to_column(row):
    return jnp.sum(jnp.where(diagonal(), row, 0.0), axis=1, keepdims=True)


def block_at(i, size):
    return pl.ds(pl.multiple_of(i * size, size), size)


def unrolled_loop(steps, by, body):
    def several(i, _):
        for u in range(by):
            body(i * by + u)
        return 0

    lax.fori_loop(0, steps // by, several, 0)


def call(kernel, outs, *args, scratch=(), limit=16, apart=()):
    def spec(a):
        if any(a is one for one in apart):
            return pl.BlockSpec(memory_space=pltpu.HBM)
        return SMEM if a.dtype == jnp.int32 else VMEM

    outs = tuple(jax.ShapeDtypeStruct(*o) for o in outs)
    return pl.pallas_call(
        kernel,
        out_shape=outs,
        in_specs=[spec(a) for a in args],
        out_specs=tuple(spec(o) for o in outs),
        scratch_shapes=[pltpu.VMEM(s, F32) if isinstance(s, tuple) else s for s in scratch],
        compiler_params=pltpu.CompilerParams(vmem_limit_bytes=limit << 20),
    )(*args)


def pack_kernel(feat_ref, out_ref):
    per_row, depth = feat_ref.shape
    width = depth * per_row
    spread = lax.broadcasted_iota(jnp.int32, (depth, width), 1) // per_row == lax.broadcasted_iota(
        jnp.int32, (depth, width), 0
    )
    wide = jnp.dot(feat_ref[...], jnp.where(spread, 1.0, 0.0).astype(BF16), preferred_element_type=F32)
    own = lax.broadcasted_iota(jnp.int32, (per_row, width), 1) % per_row == lax.broadcasted_iota(
        jnp.int32, (per_row, width), 0
    )
    line = jnp.sum(jnp.where(own, wide, 0.0), axis=0, keepdims=True)
    lines = jnp.concatenate([line[:, h * LANE : (h + 1) * LANE] for h in range(width // LANE)], axis=0)
    out_ref[...] = jnp.broadcast_to(lines.astype(BF16)[None], out_ref.shape)


def prep_kernel(
    place_ref, site_ref, pot_ref, core_pot_ref, demand_ref, core_demand_ref, far_demand_ref, cross_demand_ref,
    weight_ref, sites_ref, site_norm_ref, site_top_ref, level_ref, part_ref, log_share_ref, mix_ref,
    quarter_ref, share_ref, weights_ref, sems,
):
    n_sites = site_ref.shape[1]
    core, far = place_ref[1], place_ref[2]
    here = pl.ds(pl.multiple_of((2 * far + core) * n_sites, n_sites), n_sites)
    copies = [
        pltpu.make_async_copy(source, target, sems.at[k])
        for k, (source, target) in enumerate(
            ((pot_ref.at[:, here], quarter_ref), (demand_ref, share_ref), (weight_ref, weights_ref))
        )
    ]
    for copy in copies:
        copy.start()
    width = sites_ref.shape[0]
    depth, n_sites = site_ref.shape
    site = site_ref[...]
    wide = site.astype(F32)
    site_norm = jnp.sum(wide * wide, axis=0, keepdims=True)
    site_top_ref[...] = jnp.broadcast_to(jnp.max(site_norm, axis=1, keepdims=True), site_top_ref.shape)
    for b in range(n_sites // LANE):
        site_norm_ref[b : b + 1, :] = site_norm[:, b * LANE : (b + 1) * LANE] / (depth * EPS)
    spread = (
        lax.broadcasted_iota(jnp.int32, (width, depth), 0) // (width // depth)
        == lax.broadcasted_iota(jnp.int32, (width, depth), 1)
    )
    sites_ref[...] = jnp.dot(
        jnp.where(spread, 1.0, 0.0).astype(BF16), site, preferred_element_type=F32
    ).astype(BF16)
    for copy in copies:
        copy.wait()

    def by_core(own, other):
        return jnp.where(core == 0, own, other), jnp.where(core == 0, other, own)

    for s, line in enumerate(by_core(quarter_ref[...], core_pot_ref[:, here])):
        for b in range(n_sites // LANE):
            level_ref[s, b : b + 1, :] = line[:, b * LANE : (b + 1) * LANE]
    level = level_ref[...] * (1.0 / EPS) - site_norm_ref[...][None]
    level_ref[...] = level
    part_ref[...] = jnp.exp(level - overall(jnp.max, level))
    near = by_core(share_ref[...], core_demand_ref[...])
    away = by_core(far_demand_ref[...], cross_demand_ref[...])
    half = log_share_ref.shape[1] // 2
    for s in range(2):
        first = jnp.where(far == 0, near[s], away[s])
        second = jnp.where(far == 0, away[s], near[s])
        for b in range(half):
            log_share_ref[s, b : b + 1, :] = first[:, b * LANE : (b + 1) * LANE]
            log_share_ref[s, half + b : half + b + 1, :] = second[:, b * LANE : (b + 1) * LANE]
    demand = log_share_ref[...]
    log_share_ref[...] = jnp.log(demand) - jnp.log(overall(jnp.sum, demand))
    weight = weights_ref[...]
    which = lax.broadcasted_iota(jnp.int32, weight.shape, 1)
    total = jnp.sum(weight, axis=1, keepdims=True)
    for s in range(2):
        own = jnp.sum(jnp.where(which == 2 * place_ref[0] + s, weight, 0.0), axis=1, keepdims=True)
        mix_ref[s] = jnp.broadcast_to(own / total, mix_ref.shape[1:])


def overall(reduce, value):
    return reduce(reduce(value, axis=2, keepdims=True), axis=1, keepdims=True)


def cell_rows(i, feat, size, per_row):
    width = feat.shape[1]
    rows = lax.broadcasted_iota(jnp.int32, (size, width), 0)
    lanes = lax.broadcasted_iota(jnp.int32, (size, width), 1)
    pick = jnp.where(rows // per_row + i * (size // per_row) == lanes, 1.0, 0.0).astype(BF16)
    block = jnp.dot(pick, feat, preferred_element_type=F32)
    return jnp.where(rows % per_row == lanes % per_row, block, 0.0).astype(BF16)


def build_kernel(
    feat_ref, sites_ref, site_top_ref, level_ref, part_ref,
    gibbs_ref, cells_ref, cell_norm_ref, safe_ref, send_ref, out_ref, sum_ref,
):
    n_cells, width = cells_ref.shape
    n_sites = sites_ref.shape[1]
    n_lines = feat_ref.shape[0]
    per_row = n_cells // n_lines
    depth = width // per_row
    rows_blk, cols_blk = 512, 512
    feat = feat_ref[...]
    wide = feat.astype(F32)
    square = wide * wide
    high = square.astype(BF16)
    low = (square - high.astype(F32)).astype(BF16)
    same = lax.broadcasted_iota(jnp.int32, (width, LANE), 0) % per_row == lax.broadcasted_iota(
        jnp.int32, (width, LANE), 1
    ) % per_row
    fold = jnp.where(same, 1.0, 0.0).astype(BF16)
    norm = jnp.dot(high, fold, preferred_element_type=F32) + jnp.dot(low, fold, preferred_element_type=F32)
    group = LANE // per_row
    own = lax.broadcasted_iota(jnp.int32, (n_lines, LANE), 0) % group == lax.broadcasted_iota(
        jnp.int32, (n_lines, LANE), 1
    ) // per_row
    cell_norm_ref[...] = jnp.sum(
        jnp.where(own, norm, 0.0).reshape(n_cells // LANE, group, LANE), axis=1
    ) / (depth * EPS)
    safe = jnp.max(norm) * jnp.max(site_top_ref[...]) <= SAFE_NORMS
    safe_ref[0, 0] = jnp.where(safe, 1, 0)

    @pl.when(safe)
    def _():
        scale = 2.0 / (depth * EPS) * math.log2(math.e)

        def block(i):
            at = block_at(i, rows_blk)
            rows = cell_rows(i, feat_ref[...], rows_blk, per_row)
            for j in range(n_sites // cols_blk):
                inner = jnp.dot(
                    rows, sites_ref[:, j * cols_blk : (j + 1) * cols_blk], preferred_element_type=F32
                )
                values = jnp.exp2(inner * scale)
                gibbs_ref[at, j * cols_blk : (j + 1) * cols_blk] = values
                for s in range(2):
                    terms = [
                        values[:, b * LANE : (b + 1) * LANE]
                        * part_ref[s, j * (cols_blk // LANE) + b : j * (cols_blk // LANE) + b + 1, :]
                        for b in range(cols_blk // LANE)
                    ]
                    added = (terms[0] + terms[1]) + (terms[2] + terms[3])
                    if j == 0:
                        sum_ref[s, at, :] = added
                    else:
                        sum_ref[s, at, :] += added

        unrolled_loop(n_cells // rows_blk, 1, block)

        def fold_block(i):
            at = block_at(i, LANE)
            for s in range(2):
                out_ref[s, pl.ds(i, 1), :] = to_row(jnp.sum(sum_ref[s, at, :], axis=1, keepdims=True))

        unrolled_loop(n_cells // LANE, 8, fold_block)
        out_ref[...] = overall(jnp.max, level_ref[...]) + jnp.log(out_ref[...])

    @pl.when(jnp.logical_not(safe))
    def _():
        for i in range(n_cells // rows_blk):
            cells_ref[i * rows_blk : (i + 1) * rows_blk, :] = cell_rows(i, feat_ref[...], rows_blk, per_row)
        log_domain(level_ref[...], cells_ref, sites_ref, out_ref, True)

    send_ref[...] = jnp.broadcast_to(out_ref[...][None], send_ref.shape)


def log_domain(level, cells_ref, sites_ref, out_ref, over_sites):
    n_scen, blocks_in, _ = level.shape
    scale = 2.0 / ((cells_ref.shape[1] // 8) * EPS)

    def block(i, _):
        at = block_at(i, LANE)
        if over_sites:
            inner = jnp.dot(cells_ref[at, :], sites_ref[...], preferred_element_type=F32)
        else:
            inner = lax.dot_general(
                sites_ref[:, at], cells_ref[...], (((0,), (1,)), ((), ())), preferred_element_type=F32
            )
        for s in range(n_scen):
            score = inner * scale + jnp.concatenate([level[s, b : b + 1, :] for b in range(blocks_in)], axis=1)
            top = jnp.max(score, axis=1, keepdims=True)
            total = jnp.sum(jnp.exp(score - top), axis=1, keepdims=True)
            out_ref[s, pl.ds(i, 1), :] = to_row(top + jnp.log(total))
        return 0

    lax.fori_loop(0, out_ref.shape[1], block, 0)


def log_sums(safe, level, gibbs_ref, cells_ref, sites_ref, out_ref, part_ref, sum_ref, over_sites):
    n_scen, blocks_in, _ = level.shape
    blocks_out = out_ref.shape[1]

    @pl.when(safe)
    def _():
        top = overall(jnp.max, level)
        part_ref[...] = jnp.exp(level - top)
        if over_sites:

            def cell_block(i):
                at = block_at(i, LANE)
                sums = [jnp.zeros((LANE, LANE), F32) for _ in range(n_scen)]
                for b in range(blocks_in):
                    tile = gibbs_ref[at, b * LANE : (b + 1) * LANE]
                    for s in range(n_scen):
                        sums[s] += tile * part_ref[s, b : b + 1, :]
                for s in range(n_scen):
                    out_ref[s, pl.ds(i, 1), :] = to_row(jnp.sum(sums[s], axis=1, keepdims=True))

            unrolled_loop(blocks_out, 8, cell_block)
        else:
            sum_ref[...] = jnp.zeros_like(sum_ref)

            def cell_block(i):
                at = block_at(i, LANE)
                columns = [
                    jnp.broadcast_to(to_column(part_ref[s, pl.ds(i, 1), :]), (LANE, LANE)) for s in range(n_scen)
                ]
                for b in range(blocks_out):
                    tile = gibbs_ref[at, b * LANE : (b + 1) * LANE]
                    for s in range(n_scen):
                        sum_ref[s, b] += jnp.sum((tile * columns[s]).reshape(LANE // 8, 8, LANE), axis=0)

            unrolled_loop(blocks_in, 8, cell_block)
            out_ref[...] = jnp.sum(sum_ref[...], axis=2)
        out_ref[...] = top + jnp.log(out_ref[...])

    @pl.when(jnp.logical_not(safe))
    def _():
        log_domain(level, cells_ref, sites_ref, out_ref, over_sites)


def next_row_kernel(
    safe_ref, terms_ref, column_ref, gibbs_ref, cells_ref, sites_ref, send_ref, level_ref, out_ref, part_ref
):
    level = jnp.sum(terms_ref[...], axis=0)[None] - column_ref[...]
    level_ref[...] = level
    log_sums(safe_ref[0, 0] == 1, level, gibbs_ref, cells_ref, sites_ref, out_ref, part_ref, None, True)
    send_ref[...] = jnp.broadcast_to(out_ref[...][None], send_ref.shape)


def column_kernel(
    safe_ref, place_ref, mix_ref, log_share_ref, got_ref, cell_norm_ref, level_ref, gibbs_ref, cells_ref, sites_ref,
    send_ref, column_ref, row_pot_ref, part_ref, sum_ref,
):
    half = row_pot_ref.shape[0]
    got = got_ref[...]
    top = jnp.max(got, axis=0)
    row = top + jnp.log(jnp.sum(jnp.exp(got - top[None]), axis=0))
    down = log_share_ref[...] - row
    own = jnp.where(place_ref[1] == 0, down[0], down[1])
    norm = cell_norm_ref[...]
    first = place_ref[2] == 0
    row_pot_ref[...] = EPS * (jnp.where(first, own[:half], own[half:]) + jnp.where(first, norm[:half], norm[half:]))
    log_sums(safe_ref[0, 0] == 1, down, gibbs_ref, cells_ref, sites_ref, column_ref, part_ref, sum_ref, False)
    term = mix_ref[0] * (level_ref[0] + column_ref[0]) + mix_ref[1] * (level_ref[1] + column_ref[1])
    send_ref[...] = jnp.broadcast_to(term[None], send_ref.shape)


def last_kernel(place_ref, terms_ref, column_ref, site_norm_ref, own_ref, other_ref):
    n_blocks = site_norm_ref.shape[0]
    log_bary = jnp.sum(terms_ref[...], axis=0)
    potential = EPS * (log_bary[None] - column_ref[...] + site_norm_ref[...][None])
    first = place_ref[1] == 0
    own_ref[:n_blocks, :] = jnp.where(first, potential[0], potential[1])
    other_ref[:n_blocks, :] = jnp.where(first, potential[1], potential[0])
    own_ref[n_blocks:, :] = log_bary
    other_ref[n_blocks:, :] = log_bary


def join_kernel(place_ref, own_ref, core_ref, far_ref, cross_ref, pot_ref, log_bary_ref):
    n_blocks = own_ref.shape[0] // 2
    here = 2 * place_ref[2] + place_ref[1]
    for flip, ref in enumerate((own_ref, core_ref, far_ref, cross_ref)):
        at = block_at(here ^ flip, n_blocks)
        pot_ref[at, :] = ref[:n_blocks, :]
        log_bary_ref[at, :] = ref[n_blocks:, :]


def exchange(value, axes):
    return lax.all_to_all(value, axes, split_axis=0, concat_axis=0, tiled=True)


def swapped(value, flip):
    return lax.ppermute(value, SWAP_GROUP, [(k, k ^ flip) for k in range(4)])


def on_device(demand, start_potential, cell_feat, site_feat, weights):
    n_home = lax.axis_size(HOME_GROUP)
    n_row = lax.axis_size(ROW_GROUP)
    n_bary = lax.axis_size(BARY_GROUP)
    n_sites = start_potential.shape[1] // n_home
    n_cells = demand.shape[1] * 2
    site_blocks, cell_blocks = n_sites // LANE, n_cells // LANE
    quarter = lax.axis_index(HOME_GROUP)
    place = jnp.stack([lax.axis_index(BARY_GROUP), lax.axis_index("core"), lax.axis_index("xh")]).astype(jnp.int32)

    width = cell_feat.size
    n_all = lax.axis_size(CELL_ORDER)
    (packed,) = call(pack_kernel, [((n_all, width // LANE, LANE), BF16)], cell_feat.T)
    packed, demand, start_potential = lax.optimization_barrier((packed, demand, start_potential))
    feat = exchange(packed, CELL_ORDER)
    feat = feat.reshape(n_all, width)
    core_pot = swapped(start_potential, CORE)
    core_demand = swapped(demand, CORE)
    far_demand = swapped(demand, FAR)
    cross_demand = swapped(demand, CROSS)
    own_sites = lax.dynamic_slice_in_dim(site_feat, quarter * n_sites, n_sites, 1)
    weight = weights.reshape(1, -1)
    on_cells, on_sites = (2, cell_blocks, LANE), (2, site_blocks, LANE)
    sites, site_norm, site_top, level, part, log_share, mix = call(
        prep_kernel,
        [
            ((width, n_sites), BF16),
            ((site_blocks, LANE), F32),
            ((8, LANE), F32),
            (on_sites, F32),
            (on_sites, F32),
            (on_cells, F32),
            ((2, 1, LANE), F32),
        ],
        place, own_sites, start_potential, core_pot, demand, core_demand, far_demand, cross_demand,
        weight,
        scratch=[(1, n_sites), demand.shape, weight.shape, pltpu.SemaphoreType.DMA((3,))],
        apart=(start_potential, demand, weight),
    )
    feat, sites, site_norm, site_top, level, part, log_share, mix, place = lax.optimization_barrier(
        (feat, sites, site_norm, site_top, level, part, log_share, mix, place)
    )
    row_outs = [((n_row, *on_cells), F32), (on_sites, F32)]
    row_scratch = [on_cells, on_sites]
    gibbs, cells, cell_norm, safe, send = call(
        build_kernel,
        [
            ((n_cells, n_sites), F32),
            ((n_cells, width), BF16),
            ((cell_blocks, LANE), F32),
            ((1, 1), jnp.int32),
            row_outs[0],
        ],
        feat, sites, site_top, level, part, scratch=[on_cells, (2, n_cells, LANE)], limit=24,
    )
    for repeat in range(ITERS):
        got = exchange(send, ROW_GROUP)
        send, column, row_pot = call(
            column_kernel,
            [((n_bary, site_blocks, LANE), F32), (on_sites, F32), ((cell_blocks // 2, LANE), F32)],
            safe, place, mix, log_share, got, cell_norm, level, gibbs, cells, sites,
            scratch=[on_cells, (2, site_blocks, 8, LANE)],
        )
        terms = exchange(send, BARY_GROUP)
        if repeat < ITERS - 1:
            send, level = call(
                next_row_kernel, row_outs, safe, terms, column, gibbs, cells, sites, scratch=row_scratch
            )
    message = ((2 * site_blocks, LANE), F32)
    own, other = call(last_kernel, [message] * 2, place, terms, column, site_norm)
    whole = ((n_home * site_blocks, LANE), F32)
    potential, log_bary = call(
        join_kernel, [whole] * 2, place, own, swapped(other, CORE), swapped(own, FAR), swapped(other, CROSS)
    )
    return row_pot.reshape(1, -1), potential.reshape(1, -1), log_bary.reshape(-1)


def solution(mesh):
    torus = Mesh(
        mesh.devices.reshape(8, 4, 2, mesh.shape["cell"], mesh.shape["site"]), ("z", "y", "core", "xh", "xl")
    )
    return jax.shard_map(
        on_device,
        mesh=torus,
        in_specs=(P(SCEN, "xh"), P(SCEN, "xl"), P(None, CELL_ORDER), P(None, "xl"), P()),
        out_specs=(P(SCEN, "xh"), P(SCEN, "xl"), P("xl")),
        check_vma=False,
    )
```

```python
import math

import jax
import jax.numpy as jnp
from jax import lax
from jax.experimental import pallas as pl
from jax.experimental.pallas import tpu as pltpu
from jax.sharding import Mesh
from jax.sharding import PartitionSpec as P

ITERS = 2
EPS = 0.25
SCEN = ("z", "y", "core")
CELL_ORDER = ("xh", "z", "y", "core", "xl")
ROW_GROUP = ("xh", "xl", "core")
BARY_GROUP = ("z", "y")
HOME_GROUP = ("xh", "core")
SWAP_GROUP = ("core", "xh")
CORE, FAR, CROSS = 2, 1, 3
F32 = jnp.float32
BF16 = jnp.bfloat16
SAFE_NORMS = 14400.0
LANE = 128
VMEM = pl.BlockSpec(memory_space=pltpu.VMEM)
SMEM = pl.BlockSpec(memory_space=pltpu.SMEM)
HBM = pl.BlockSpec(memory_space=pltpu.HBM)


def diagonal():
    shape = (LANE, LANE)
    return lax.broadcasted_iota(jnp.int32, shape, 0) == lax.broadcasted_iota(jnp.int32, shape, 1)


def to_row(column):
    return jnp.sum(jnp.where(diagonal(), column, 0.0), axis=0, keepdims=True)


def to_column(row):
    return jnp.sum(jnp.where(diagonal(), row, 0.0), axis=1, keepdims=True)


def block_at(i, size):
    return pl.ds(pl.multiple_of(i * size, size), size)


def unrolled_loop(steps, by, body):
    def several(i, _):
        for u in range(by):
            body(i * by + u)
        return 0

    lax.fori_loop(0, steps // by, several, 0)


def in_hbm(value):
    return pltpu.with_memory_space_constraint(value, pltpu.HBM)


def call(kernel, outs, *args, scratch=(), limit=16, apart=()):
    def spec(a):
        return SMEM if a.dtype == jnp.int32 else VMEM

    outs = tuple(jax.ShapeDtypeStruct(*o) for o in outs)
    return pl.pallas_call(
        kernel,
        out_shape=outs,
        in_specs=[HBM if k in apart else spec(a) for k, a in enumerate(args)],
        out_specs=tuple(spec(o) for o in outs),
        scratch_shapes=[pltpu.VMEM(s, F32) if isinstance(s, tuple) else s for s in scratch],
        compiler_params=pltpu.CompilerParams(vmem_limit_bytes=limit << 20),
    )(*args)


def pack_kernel(feat_ref, out_ref):
    per_row, depth = feat_ref.shape
    width = depth * per_row
    spread = lax.broadcasted_iota(jnp.int32, (depth, width), 1) // per_row == lax.broadcasted_iota(
        jnp.int32, (depth, width), 0
    )
    wide = jnp.dot(feat_ref[...], jnp.where(spread, 1.0, 0.0).astype(BF16), preferred_element_type=F32)
    own = lax.broadcasted_iota(jnp.int32, (per_row, width), 1) % per_row == lax.broadcasted_iota(
        jnp.int32, (per_row, width), 0
    )
    line = jnp.sum(jnp.where(own, wide, 0.0), axis=0, keepdims=True)
    lines = jnp.concatenate([line[:, h * LANE : (h + 1) * LANE] for h in range(width // LANE)], axis=0)
    out_ref[...] = jnp.broadcast_to(lines.astype(BF16)[None], out_ref.shape)


def prep_kernel(
    place_ref, site_ref, pot_ref, core_pot_ref, weight_ref, demand_ref,
    sites_ref, site_norm_ref, site_top_ref, level_ref, part_ref, mix_ref, share_ref, spot_ref,
    quarter_ref, weights_ref, line_ref, sems,
):
    width = sites_ref.shape[0]
    depth, n_sites = site_ref.shape
    core, far = place_ref[1], place_ref[2]
    here = pl.ds(pl.multiple_of((2 * far + core) * n_sites, n_sites), n_sites)
    copies = [
        pltpu.make_async_copy(pot_ref.at[:, here], quarter_ref, sems.at[0]),
        pltpu.make_async_copy(weight_ref, weights_ref, sems.at[1]),
        pltpu.make_async_copy(demand_ref, line_ref, sems.at[2]),
    ]
    for copy in copies:
        copy.start()
    site = site_ref[...]
    wide = site.astype(F32)
    site_norm = jnp.sum(wide * wide, axis=0, keepdims=True)
    site_top_ref[...] = jnp.broadcast_to(jnp.max(site_norm, axis=1, keepdims=True), site_top_ref.shape)
    for b in range(n_sites // LANE):
        site_norm_ref[b : b + 1, :] = site_norm[:, b * LANE : (b + 1) * LANE] / (depth * EPS)
    spread = (
        lax.broadcasted_iota(jnp.int32, (width, depth), 0) // (width // depth)
        == lax.broadcasted_iota(jnp.int32, (width, depth), 1)
    )
    sites_ref[...] = jnp.dot(
        jnp.where(spread, 1.0, 0.0).astype(BF16), site, preferred_element_type=F32
    ).astype(BF16)
    for copy in copies:
        copy.wait()
    for s, line in enumerate(by_core(core, quarter_ref[...], core_pot_ref[:, here])):
        for b in range(n_sites // LANE):
            level_ref[s, b : b + 1, :] = line[:, b * LANE : (b + 1) * LANE]
    level = level_ref[...] * (1.0 / EPS) - site_norm_ref[...][None]
    level_ref[...] = level
    part_ref[...] = jnp.exp(level - overall(jnp.max, level))
    for k, bit in enumerate((core, far)):
        spot_ref[k] = jnp.full(spot_ref.shape[1:], bit, jnp.int32).astype(F32)
    for b in range(share_ref.shape[0]):
        share_ref[b : b + 1, :] = line_ref[:, b * LANE : (b + 1) * LANE]
    weight = weights_ref[...]
    which = lax.broadcasted_iota(jnp.int32, weight.shape, 1)
    total = jnp.sum(weight, axis=1, keepdims=True)
    for s in range(2):
        own = jnp.sum(jnp.where(which == 2 * place_ref[0] + s, weight, 0.0), axis=1, keepdims=True)
        mix_ref[s] = jnp.broadcast_to(own / total, mix_ref.shape[1:])


def by_core(core, own, other):
    return jnp.where(core == 0, own, other), jnp.where(core == 0, other, own)


def overall(reduce, value):
    return reduce(reduce(value, axis=2, keepdims=True), axis=1, keepdims=True)


def cell_rows(i, feat, size, per_row):
    width = feat.shape[1]
    rows = lax.broadcasted_iota(jnp.int32, (size, width), 0)
    lanes = lax.broadcasted_iota(jnp.int32, (size, width), 1)
    pick = jnp.where(rows // per_row + i * (size // per_row) == lanes, 1.0, 0.0).astype(BF16)
    block = jnp.dot(pick, feat, preferred_element_type=F32)
    return jnp.where(rows % per_row == lanes % per_row, block, 0.0).astype(BF16)


def build_kernel(
    feat_ref, sites_ref, site_top_ref, level_ref, part_ref, share_ref,
    gibbs_ref, cells_ref, cell_norm_ref, safe_ref, send_ref, out_ref, sum_ref,
):
    n_cells, width = cells_ref.shape
    n_sites = sites_ref.shape[1]
    n_lines = feat_ref.shape[0]
    per_row = n_cells // n_lines
    depth = width // per_row
    rows_blk, cols_blk = 512, 512
    feat = feat_ref[...]
    wide = feat.astype(F32)
    square = wide * wide
    high = square.astype(BF16)
    low = (square - high.astype(F32)).astype(BF16)
    same = lax.broadcasted_iota(jnp.int32, (width, LANE), 0) % per_row == lax.broadcasted_iota(
        jnp.int32, (width, LANE), 1
    ) % per_row
    fold = jnp.where(same, 1.0, 0.0).astype(BF16)
    norm = jnp.dot(high, fold, preferred_element_type=F32) + jnp.dot(low, fold, preferred_element_type=F32)
    group = LANE // per_row
    own = lax.broadcasted_iota(jnp.int32, (n_lines, LANE), 0) % group == lax.broadcasted_iota(
        jnp.int32, (n_lines, LANE), 1
    ) // per_row
    cell_norm_ref[...] = jnp.sum(
        jnp.where(own, norm, 0.0).reshape(n_cells // LANE, group, LANE), axis=1
    ) / (depth * EPS)
    safe = jnp.max(norm) * jnp.max(site_top_ref[...]) <= SAFE_NORMS
    safe_ref[...] = jnp.full(safe_ref.shape, jnp.where(safe, 1.0, 0.0), F32)

    @pl.when(safe)
    def _():
        scale = 2.0 / (depth * EPS) * math.log2(math.e)

        def block(i):
            at = block_at(i, rows_blk)
            rows = cell_rows(i, feat_ref[...], rows_blk, per_row)
            for j in range(n_sites // cols_blk):
                inner = jnp.dot(
                    rows, sites_ref[:, j * cols_blk : (j + 1) * cols_blk], preferred_element_type=F32
                )
                values = jnp.exp2(inner * scale)
                gibbs_ref[at, j * cols_blk : (j + 1) * cols_blk] = values
                for s in range(2):
                    terms = [
                        values[:, b * LANE : (b + 1) * LANE]
                        * part_ref[s, j * (cols_blk // LANE) + b : j * (cols_blk // LANE) + b + 1, :]
                        for b in range(cols_blk // LANE)
                    ]
                    added = (terms[0] + terms[1]) + (terms[2] + terms[3])
                    if j == 0:
                        sum_ref[s, at, :] = added
                    else:
                        sum_ref[s, at, :] += added

        unrolled_loop(n_cells // rows_blk, 1, block)

        def fold_block(i):
            at = block_at(i, LANE)
            for s in range(2):
                out_ref[s, pl.ds(i, 1), :] = to_row(jnp.sum(sum_ref[s, at, :], axis=1, keepdims=True))

        unrolled_loop(n_cells // LANE, 8, fold_block)
        out_ref[...] = overall(jnp.max, level_ref[...]) + jnp.log(out_ref[...])

    @pl.when(jnp.logical_not(safe))
    def _():
        for i in range(n_cells // rows_blk):
            cells_ref[i * rows_blk : (i + 1) * rows_blk, :] = cell_rows(i, feat_ref[...], rows_blk, per_row)
        log_domain(level_ref[...], cells_ref, sites_ref, out_ref, True)

    flat = out_ref.shape[0] * out_ref.shape[1]
    send_ref[:, :flat, :] = jnp.broadcast_to(out_ref[...].reshape(1, flat, LANE), (send_ref.shape[0], flat, LANE))
    send_ref[:, flat:, :] = jnp.broadcast_to(share_ref[...][None], (send_ref.shape[0], *share_ref.shape))


def log_domain(level, cells_ref, sites_ref, out_ref, over_sites):
    n_scen, blocks_in, _ = level.shape
    scale = 2.0 / ((cells_ref.shape[1] // 8) * EPS)

    def block(i, _):
        at = block_at(i, LANE)
        if over_sites:
            inner = jnp.dot(cells_ref[at, :], sites_ref[...], preferred_element_type=F32)
        else:
            inner = lax.dot_general(
                sites_ref[:, at], cells_ref[...], (((0,), (1,)), ((), ())), preferred_element_type=F32
            )
        for s in range(n_scen):
            score = inner * scale + jnp.concatenate([level[s, b : b + 1, :] for b in range(blocks_in)], axis=1)
            top = jnp.max(score, axis=1, keepdims=True)
            total = jnp.sum(jnp.exp(score - top), axis=1, keepdims=True)
            out_ref[s, pl.ds(i, 1), :] = to_row(top + jnp.log(total))
        return 0

    lax.fori_loop(0, out_ref.shape[1], block, 0)


def log_sums(safe, level, gibbs_ref, cells_ref, sites_ref, out_ref, part_ref, sum_ref, over_sites):
    n_scen, blocks_in, _ = level.shape
    blocks_out = out_ref.shape[1]

    @pl.when(safe)
    def _():
        top = overall(jnp.max, level)
        part_ref[...] = jnp.exp(level - top)
        if over_sites:

            def cell_block(i):
                at = block_at(i, LANE)
                sums = [jnp.zeros((LANE, LANE), F32) for _ in range(n_scen)]
                for b in range(blocks_in):
                    tile = gibbs_ref[at, b * LANE : (b + 1) * LANE]
                    for s in range(n_scen):
                        sums[s] += tile * part_ref[s, b : b + 1, :]
                for s in range(n_scen):
                    out_ref[s, pl.ds(i, 1), :] = to_row(jnp.sum(sums[s], axis=1, keepdims=True))

            unrolled_loop(blocks_out, 8, cell_block)
        else:
            sum_ref[...] = jnp.zeros_like(sum_ref)

            def cell_block(i):
                at = block_at(i, LANE)
                columns = [
                    jnp.broadcast_to(to_column(part_ref[s, pl.ds(i, 1), :]), (LANE, LANE)) for s in range(n_scen)
                ]
                for b in range(blocks_out):
                    tile = gibbs_ref[at, b * LANE : (b + 1) * LANE]
                    for s in range(n_scen):
                        sum_ref[s, b] += jnp.sum((tile * columns[s]).reshape(LANE // 8, 8, LANE), axis=0)

            unrolled_loop(blocks_in, 8, cell_block)
            out_ref[...] = jnp.sum(sum_ref[...], axis=2)
        out_ref[...] = top + jnp.log(out_ref[...])

    @pl.when(jnp.logical_not(safe))
    def _():
        log_domain(level, cells_ref, sites_ref, out_ref, over_sites)


def next_row_kernel(
    safe_ref, terms_ref, column_ref, gibbs_ref, cells_ref, sites_ref, send_ref, level_ref, out_ref, part_ref
):
    level = jnp.sum(terms_ref[...], axis=0)[None] - column_ref[...]
    level_ref[...] = level
    log_sums(jnp.max(safe_ref[...]) > 0.5, level, gibbs_ref, cells_ref, sites_ref, out_ref, part_ref, None, True)
    send_ref[...] = jnp.broadcast_to(out_ref[...][None], send_ref.shape)


def over_peers(got):
    top = jnp.max(got, axis=0)
    return top + jnp.log(jnp.sum(jnp.exp(got - top[None]), axis=0))


def send_term(mix_ref, level_ref, column_ref, send_ref):
    term = mix_ref[0] * (level_ref[0] + column_ref[0]) + mix_ref[1] * (level_ref[1] + column_ref[1])
    send_ref[...] = jnp.broadcast_to(term[None], send_ref.shape)


def first_column_kernel(
    safe_ref, mix_ref, got_ref, level_ref, gibbs_ref, cells_ref, sites_ref,
    send_ref, column_ref, log_share_ref, part_ref, sum_ref,
):
    on_cells = log_share_ref.shape
    flat = on_cells[0] * on_cells[1]
    near, away = 0, got_ref.shape[0] // 2
    for s in range(2):
        log_share_ref[s] = jnp.concatenate([got_ref[near + s, flat:, :], got_ref[away + s, flat:, :]], axis=0)
    demand = log_share_ref[...]
    log_share = jnp.log(demand) - jnp.log(overall(jnp.sum, demand))
    log_share_ref[...] = log_share
    down = log_share - over_peers(got_ref[:, :flat, :]).reshape(on_cells)
    log_sums(jnp.max(safe_ref[...]) > 0.5, down, gibbs_ref, cells_ref, sites_ref, column_ref, part_ref, sum_ref, False)
    send_term(mix_ref, level_ref, column_ref, send_ref)


def next_column_kernel(
    safe_ref, spot_ref, mix_ref, log_share_ref, got_ref, cell_norm_ref, level_ref, gibbs_ref, cells_ref, sites_ref,
    send_ref, column_ref, row_pot_ref, part_ref, sum_ref,
):
    half = row_pot_ref.shape[0]
    down = log_share_ref[...] - over_peers(got_ref[...])
    own = jnp.where(spot_ref[0] == 0.0, down[0], down[1])
    norm = cell_norm_ref[...]
    first = spot_ref[1] == 0.0
    row_pot_ref[...] = EPS * (jnp.where(first, own[:half], own[half:]) + jnp.where(first, norm[:half], norm[half:]))
    log_sums(jnp.max(safe_ref[...]) > 0.5, down, gibbs_ref, cells_ref, sites_ref, column_ref, part_ref, sum_ref, False)
    send_term(mix_ref, level_ref, column_ref, send_ref)


def last_kernel(spot_ref, terms_ref, column_ref, site_norm_ref, own_ref, other_ref):
    n_blocks = site_norm_ref.shape[0]
    log_bary = jnp.sum(terms_ref[...], axis=0)
    potential = EPS * (log_bary[None] - column_ref[...] + site_norm_ref[...][None])
    first = spot_ref[0] == 0.0
    own_ref[:n_blocks, :] = jnp.where(first, potential[0], potential[1])
    other_ref[:n_blocks, :] = jnp.where(first, potential[1], potential[0])
    own_ref[n_blocks:, :] = log_bary
    other_ref[n_blocks:, :] = log_bary


def exchange(value, axes):
    return lax.all_to_all(value, axes, split_axis=0, concat_axis=0, tiled=True)


def swapped(value, flip):
    return lax.ppermute(value, SWAP_GROUP, [(k, k ^ flip) for k in range(4)])


def on_device(demand, start_potential, cell_feat, site_feat, weights):
    n_home = lax.axis_size(HOME_GROUP)
    n_row = lax.axis_size(ROW_GROUP)
    n_bary = lax.axis_size(BARY_GROUP)
    n_sites = start_potential.shape[1] // n_home
    n_cells = demand.shape[1] * 2
    site_blocks, cell_blocks = n_sites // LANE, n_cells // LANE
    quarter = lax.axis_index(HOME_GROUP)
    place = jnp.stack([lax.axis_index(BARY_GROUP), lax.axis_index("core"), lax.axis_index("xh")]).astype(jnp.int32)

    width = cell_feat.size
    n_all = lax.axis_size(CELL_ORDER)
    (packed,) = call(pack_kernel, [((n_all, width // LANE, LANE), BF16)], cell_feat.T)
    packed, demand, start_potential = lax.optimization_barrier((packed, demand, start_potential))
    feat = exchange(packed, CELL_ORDER)
    feat = feat.reshape(n_all, width)
    core_pot = swapped(start_potential, CORE)
    own_sites = lax.dynamic_slice_in_dim(site_feat, quarter * n_sites, n_sites, 1)
    weight = weights.reshape(1, -1)
    on_cells, on_sites = (2, cell_blocks, LANE), (2, site_blocks, LANE)
    sites, site_norm, site_top, level, part, mix, share, spot = call(
        prep_kernel,
        [
            ((width, n_sites), BF16),
            ((site_blocks, LANE), F32),
            ((8, LANE), F32),
            (on_sites, F32),
            (on_sites, F32),
            ((2, 1, LANE), F32),
            ((cell_blocks // 2, LANE), F32),
            ((2, 1, LANE), F32),
        ],
        place, own_sites, in_hbm(start_potential), core_pot, in_hbm(weight), in_hbm(demand),
        scratch=[(1, n_sites), weight.shape, demand.shape, pltpu.SemaphoreType.DMA((3,))],
        apart=(2, 4, 5),
    )
    feat, sites, site_norm, site_top, level, part, mix, share, spot = lax.optimization_barrier(
        (feat, sites, site_norm, site_top, level, part, mix, share, spot)
    )
    row_outs = [((n_row, *on_cells), F32), (on_sites, F32)]
    row_scratch = [on_cells, on_sites]
    gibbs, cells, cell_norm, safe, send = call(
        build_kernel,
        [
            ((n_cells, n_sites), F32),
            ((n_cells, width), BF16),
            ((cell_blocks, LANE), F32),
            ((8, LANE), F32),
            ((n_row, 2 * cell_blocks + cell_blocks // 2, LANE), F32),
        ],
        feat, sites, site_top, level, part, share, scratch=[on_cells, (2, n_cells, LANE)], limit=24,
    )
    for repeat in range(ITERS):
        got = exchange(send, ROW_GROUP)
        column_outs = [((n_bary, site_blocks, LANE), F32), (on_sites, F32)]
        column_scratch = [on_cells, (2, site_blocks, 8, LANE)]
        if repeat == 0:
            send, column, log_share = call(
                first_column_kernel, [*column_outs, (on_cells, F32)],
                safe, mix, got, level, gibbs, cells, sites, scratch=column_scratch,
            )
        else:
            send, column, row_pot = call(
                next_column_kernel, [*column_outs, ((cell_blocks // 2, LANE), F32)],
                safe, spot, mix, log_share, got, cell_norm, level, gibbs, cells, sites, scratch=column_scratch,
            )
        terms = exchange(send, BARY_GROUP)
        if repeat < ITERS - 1:
            send, level = call(
                next_row_kernel, row_outs, safe, terms, column, gibbs, cells, sites, scratch=row_scratch
            )
    message = ((2 * site_blocks, LANE), F32)
    own, other = call(last_kernel, [message] * 2, spot, terms, column, site_norm)
    pieces = (own, swapped(other, CORE), swapped(own, FAR), swapped(other, CROSS))
    here = lax.axis_index(HOME_GROUP)
    ordered = [lax.select_n(here ^ k, *pieces) for k in range(n_home)]
    potential = jnp.stack([piece[:site_blocks] for piece in ordered])
    log_bary = jnp.stack([piece[site_blocks:] for piece in ordered])
    return row_pot.reshape(1, -1), potential.reshape(1, -1), log_bary.reshape(-1)


def solution(mesh):
    torus = Mesh(
        mesh.devices.reshape(8, 4, 2, mesh.shape["cell"], mesh.shape["site"]), ("z", "y", "core", "xh", "xl")
    )
    return jax.shard_map(
        on_device,
        mesh=torus,
        in_specs=(P(SCEN, "xh"), P(SCEN, "xl"), P(None, CELL_ORDER), P(None, "xl"), P()),
        out_specs=(P(SCEN, "xh"), P(SCEN, "xl"), P("xl")),
        check_vma=False,
    )
```

```python
import math

import jax
import jax.numpy as jnp
from jax import lax
from jax.experimental import pallas as pl
from jax.experimental.pallas import tpu as pltpu
from jax.sharding import Mesh
from jax.sharding import PartitionSpec as P

ITERS = 2
EPS = 0.25
SCEN = ("z", "y", "core")
CELL_ORDER = ("xh", "z", "y", "core", "xl")
ROW_GROUP = ("xh", "xl", "core")
BARY_GROUP = ("z", "y")
HOME_GROUP = ("xh", "core")
SWAP_GROUP = ("core", "xh")
CORE, FAR, CROSS = 2, 1, 3
F32 = jnp.float32
BF16 = jnp.bfloat16
SAFE_NORMS = 14400.0
LANE = 128
VMEM = pl.BlockSpec(memory_space=pltpu.VMEM)
SMEM = pl.BlockSpec(memory_space=pltpu.SMEM)
HBM = pl.BlockSpec(memory_space=pltpu.HBM)


def diagonal():
    shape = (LANE, LANE)
    return lax.broadcasted_iota(jnp.int32, shape, 0) == lax.broadcasted_iota(jnp.int32, shape, 1)


def to_row(column):
    return jnp.sum(jnp.where(diagonal(), column, 0.0), axis=0, keepdims=True)


def to_column(row):
    return jnp.sum(jnp.where(diagonal(), row, 0.0), axis=1, keepdims=True)


def block_at(i, size):
    return pl.ds(pl.multiple_of(i * size, size), size)


def unrolled_loop(steps, by, body):
    def several(i, _):
        for u in range(by):
            body(i * by + u)
        return 0

    lax.fori_loop(0, steps // by, several, 0)


def in_hbm(value):
    return pltpu.with_memory_space_constraint(value, pltpu.HBM)


def call(kernel, outs, *args, scratch=(), limit=16, apart=()):
    def spec(a):
        return SMEM if a.dtype == jnp.int32 else VMEM

    outs = tuple(jax.ShapeDtypeStruct(*o) for o in outs)
    return pl.pallas_call(
        kernel,
        out_shape=outs,
        in_specs=[HBM if k in apart else spec(a) for k, a in enumerate(args)],
        out_specs=tuple(spec(o) for o in outs),
        scratch_shapes=[pltpu.VMEM(s, F32) if isinstance(s, tuple) else s for s in scratch],
        compiler_params=pltpu.CompilerParams(vmem_limit_bytes=limit << 20),
    )(*args)


def pack_kernel(feat_ref, out_ref):
    per_row, depth = feat_ref.shape
    width = depth * per_row
    spread = lax.broadcasted_iota(jnp.int32, (depth, width), 1) // per_row == lax.broadcasted_iota(
        jnp.int32, (depth, width), 0
    )
    wide = jnp.dot(feat_ref[...], jnp.where(spread, 1.0, 0.0).astype(BF16), preferred_element_type=F32)
    own = lax.broadcasted_iota(jnp.int32, (per_row, width), 1) % per_row == lax.broadcasted_iota(
        jnp.int32, (per_row, width), 0
    )
    line = jnp.sum(jnp.where(own, wide, 0.0), axis=0, keepdims=True)
    lines = jnp.concatenate([line[:, h * LANE : (h + 1) * LANE] for h in range(width // LANE)], axis=0)
    out_ref[...] = jnp.broadcast_to(lines.astype(BF16)[None], out_ref.shape)


def prep_kernel(
    place_ref, site_ref, pot_ref, core_pot_ref, weight_ref, demand_ref,
    sites_ref, site_norm_ref, site_top_ref, level_ref, part_ref, mix_ref, share_ref, spot_ref,
    quarter_ref, weights_ref, line_ref, sems,
):
    width = sites_ref.shape[0]
    depth, n_sites = site_ref.shape
    core, far = place_ref[1], place_ref[2]
    here = pl.ds(pl.multiple_of((2 * far + core) * n_sites, n_sites), n_sites)
    copies = [
        pltpu.make_async_copy(pot_ref.at[:, here], quarter_ref, sems.at[0]),
        pltpu.make_async_copy(weight_ref, weights_ref, sems.at[1]),
        pltpu.make_async_copy(demand_ref, line_ref, sems.at[2]),
    ]
    for copy in copies:
        copy.start()
    site = site_ref[...]
    wide = site.astype(F32)
    site_norm = jnp.sum(wide * wide, axis=0, keepdims=True)
    site_top_ref[...] = jnp.broadcast_to(jnp.max(site_norm, axis=1, keepdims=True), site_top_ref.shape)
    for b in range(n_sites // LANE):
        site_norm_ref[b : b + 1, :] = site_norm[:, b * LANE : (b + 1) * LANE] / (depth * EPS)
    spread = (
        lax.broadcasted_iota(jnp.int32, (width, depth), 0) // (width // depth)
        == lax.broadcasted_iota(jnp.int32, (width, depth), 1)
    )
    sites_ref[...] = jnp.dot(
        jnp.where(spread, 1.0, 0.0).astype(BF16), site, preferred_element_type=F32
    ).astype(BF16)
    for copy in copies:
        copy.wait()
    for s, line in enumerate(by_core(core, quarter_ref[...], core_pot_ref[:, here])):
        for b in range(n_sites // LANE):
            level_ref[s, b : b + 1, :] = line[:, b * LANE : (b + 1) * LANE]
    level = level_ref[...] * (1.0 / EPS) - site_norm_ref[...][None]
    level_ref[...] = level
    part_ref[...] = jnp.exp(level - overall(jnp.max, level))
    for k, bit in enumerate((core, far)):
        spot_ref[k] = jnp.full(spot_ref.shape[1:], bit, jnp.int32).astype(F32)
    for b in range(share_ref.shape[0]):
        share_ref[b : b + 1, :] = line_ref[:, b * LANE : (b + 1) * LANE]
    weight = weights_ref[...]
    which = lax.broadcasted_iota(jnp.int32, weight.shape, 1)
    total = jnp.sum(weight, axis=1, keepdims=True)
    for s in range(2):
        own = jnp.sum(jnp.where(which == 2 * place_ref[0] + s, weight, 0.0), axis=1, keepdims=True)
        mix_ref[s] = jnp.broadcast_to(own / total, mix_ref.shape[1:])


def by_core(core, own, other):
    return jnp.where(core == 0, own, other), jnp.where(core == 0, other, own)


def overall(reduce, value):
    return reduce(reduce(value, axis=2, keepdims=True), axis=1, keepdims=True)


def cell_rows(i, feat, size, per_row):
    width = feat.shape[1]
    rows = lax.broadcasted_iota(jnp.int32, (size, width), 0)
    lanes = lax.broadcasted_iota(jnp.int32, (size, width), 1)
    pick = jnp.where(rows // per_row + i * (size // per_row) == lanes, 1.0, 0.0).astype(BF16)
    block = jnp.dot(pick, feat, preferred_element_type=F32)
    return jnp.where(rows % per_row == lanes % per_row, block, 0.0).astype(BF16)


def build_kernel(
    feat_ref, sites_ref, site_top_ref, level_ref, part_ref, share_ref,
    gibbs_ref, cells_ref, cell_norm_ref, safe_ref, send_ref, out_ref, sum_ref,
):
    n_cells, width = cells_ref.shape
    n_sites = sites_ref.shape[1]
    n_lines = feat_ref.shape[0]
    per_row = n_cells // n_lines
    depth = width // per_row
    rows_blk, cols_blk = 512, 512
    feat = feat_ref[...]
    wide = feat.astype(F32)
    square = wide * wide
    high = square.astype(BF16)
    low = (square - high.astype(F32)).astype(BF16)
    same = lax.broadcasted_iota(jnp.int32, (width, LANE), 0) % per_row == lax.broadcasted_iota(
        jnp.int32, (width, LANE), 1
    ) % per_row
    fold = jnp.where(same, 1.0, 0.0).astype(BF16)
    norm = jnp.dot(high, fold, preferred_element_type=F32) + jnp.dot(low, fold, preferred_element_type=F32)
    group = LANE // per_row
    own = lax.broadcasted_iota(jnp.int32, (n_lines, LANE), 0) % group == lax.broadcasted_iota(
        jnp.int32, (n_lines, LANE), 1
    ) // per_row
    cell_norm_ref[...] = jnp.sum(
        jnp.where(own, norm, 0.0).reshape(n_cells // LANE, group, LANE), axis=1
    ) / (depth * EPS)
    safe = jnp.max(norm) * jnp.max(site_top_ref[...]) <= SAFE_NORMS
    safe_ref[...] = jnp.full(safe_ref.shape, jnp.where(safe, 1.0, 0.0), F32)

    @pl.when(safe)
    def _():
        scale = 2.0 / (depth * EPS) * math.log2(math.e)

        def block(i):
            at = block_at(i, rows_blk)
            rows = cell_rows(i, feat_ref[...], rows_blk, per_row)
            for j in range(n_sites // cols_blk):
                inner = jnp.dot(
                    rows, sites_ref[:, j * cols_blk : (j + 1) * cols_blk], preferred_element_type=F32
                )
                values = jnp.exp2(inner * scale)
                gibbs_ref[at, j * cols_blk : (j + 1) * cols_blk] = values
                for s in range(2):
                    terms = [
                        values[:, b * LANE : (b + 1) * LANE]
                        * part_ref[s, j * (cols_blk // LANE) + b : j * (cols_blk // LANE) + b + 1, :]
                        for b in range(cols_blk // LANE)
                    ]
                    added = (terms[0] + terms[1]) + (terms[2] + terms[3])
                    if j == 0:
                        sum_ref[s, at, :] = added
                    else:
                        sum_ref[s, at, :] += added

        unrolled_loop(n_cells // rows_blk, 1, block)

        def fold_block(i):
            at = block_at(i, LANE)
            for s in range(2):
                out_ref[s, pl.ds(i, 1), :] = to_row(jnp.sum(sum_ref[s, at, :], axis=1, keepdims=True))

        unrolled_loop(n_cells // LANE, 8, fold_block)
        out_ref[...] = overall(jnp.max, level_ref[...]) + jnp.log(out_ref[...])

    @pl.when(jnp.logical_not(safe))
    def _():
        for i in range(n_cells // rows_blk):
            cells_ref[i * rows_blk : (i + 1) * rows_blk, :] = cell_rows(i, feat_ref[...], rows_blk, per_row)
        log_domain(level_ref[...], cells_ref, sites_ref, out_ref, True)

    flat = out_ref.shape[0] * out_ref.shape[1]
    send_ref[:, :flat, :] = jnp.broadcast_to(out_ref[...].reshape(1, flat, LANE), (send_ref.shape[0], flat, LANE))
    send_ref[:, flat:, :] = jnp.broadcast_to(share_ref[...][None], (send_ref.shape[0], *share_ref.shape))


def log_domain(level, cells_ref, sites_ref, out_ref, over_sites):
    n_scen, blocks_in, _ = level.shape
    scale = 2.0 / ((cells_ref.shape[1] // 8) * EPS)

    def block(i, _):
        at = block_at(i, LANE)
        if over_sites:
            inner = jnp.dot(cells_ref[at, :], sites_ref[...], preferred_element_type=F32)
        else:
            inner = lax.dot_general(
                sites_ref[:, at], cells_ref[...], (((0,), (1,)), ((), ())), preferred_element_type=F32
            )
        for s in range(n_scen):
            score = inner * scale + jnp.concatenate([level[s, b : b + 1, :] for b in range(blocks_in)], axis=1)
            top = jnp.max(score, axis=1, keepdims=True)
            total = jnp.sum(jnp.exp(score - top), axis=1, keepdims=True)
            out_ref[s, pl.ds(i, 1), :] = to_row(top + jnp.log(total))
        return 0

    lax.fori_loop(0, out_ref.shape[1], block, 0)


def log_sums(safe, level, gibbs_ref, cells_ref, sites_ref, out_ref, part_ref, sum_ref, over_sites):
    n_scen, blocks_in, _ = level.shape
    blocks_out = out_ref.shape[1]

    @pl.when(safe)
    def _():
        top = overall(jnp.max, level)
        part_ref[...] = jnp.exp(level - top)
        if over_sites:

            def cell_block(i):
                at = block_at(i, LANE)
                sums = [jnp.zeros((LANE, LANE), F32) for _ in range(n_scen)]
                for b in range(blocks_in):
                    tile = gibbs_ref[at, b * LANE : (b + 1) * LANE]
                    for s in range(n_scen):
                        sums[s] += tile * part_ref[s, b : b + 1, :]
                for s in range(n_scen):
                    out_ref[s, pl.ds(i, 1), :] = to_row(jnp.sum(sums[s], axis=1, keepdims=True))

            unrolled_loop(blocks_out, 8, cell_block)
        else:
            sum_ref[...] = jnp.zeros_like(sum_ref)

            def cell_block(i):
                at = block_at(i, LANE)
                columns = [
                    jnp.broadcast_to(to_column(part_ref[s, pl.ds(i, 1), :]), (LANE, LANE)) for s in range(n_scen)
                ]
                for b in range(blocks_out):
                    tile = gibbs_ref[at, b * LANE : (b + 1) * LANE]
                    for s in range(n_scen):
                        sum_ref[s, b] += jnp.sum((tile * columns[s]).reshape(LANE // 8, 8, LANE), axis=0)

            unrolled_loop(blocks_in, 8, cell_block)
            out_ref[...] = jnp.sum(sum_ref[...], axis=2)
        out_ref[...] = top + jnp.log(out_ref[...])

    @pl.when(jnp.logical_not(safe))
    def _():
        log_domain(level, cells_ref, sites_ref, out_ref, over_sites)


def next_row_kernel(
    safe_ref, terms_ref, column_ref, gibbs_ref, cells_ref, sites_ref, send_ref, level_ref, out_ref, part_ref
):
    level = jnp.sum(terms_ref[...], axis=0)[None] - column_ref[...]
    level_ref[...] = level
    log_sums(jnp.max(safe_ref[...]) > 0.5, level, gibbs_ref, cells_ref, sites_ref, out_ref, part_ref, None, True)
    send_ref[...] = jnp.broadcast_to(out_ref[...][None], send_ref.shape)


def over_peers(got):
    top = jnp.max(got, axis=0)
    return top + jnp.log(jnp.sum(jnp.exp(got - top[None]), axis=0))


def send_term(mix_ref, level_ref, column_ref, send_ref):
    term = mix_ref[0] * (level_ref[0] + column_ref[0]) + mix_ref[1] * (level_ref[1] + column_ref[1])
    send_ref[...] = jnp.broadcast_to(term[None], send_ref.shape)


def first_column_kernel(
    safe_ref, mix_ref, got_ref, level_ref, gibbs_ref, cells_ref, sites_ref,
    send_ref, column_ref, log_share_ref, part_ref, sum_ref,
):
    on_cells = log_share_ref.shape
    flat = on_cells[0] * on_cells[1]
    near, away = 0, got_ref.shape[0] // 2
    for s in range(2):
        log_share_ref[s] = jnp.concatenate([got_ref[near + s, flat:, :], got_ref[away + s, flat:, :]], axis=0)
    demand = log_share_ref[...]
    log_share = jnp.log(demand) - jnp.log(overall(jnp.sum, demand))
    log_share_ref[...] = log_share
    down = log_share - over_peers(got_ref[:, :flat, :]).reshape(on_cells)
    log_sums(jnp.max(safe_ref[...]) > 0.5, down, gibbs_ref, cells_ref, sites_ref, column_ref, part_ref, sum_ref, False)
    send_term(mix_ref, level_ref, column_ref, send_ref)


def next_column_kernel(
    safe_ref, spot_ref, mix_ref, log_share_ref, got_ref, cell_norm_ref, level_ref, gibbs_ref, cells_ref, sites_ref,
    send_ref, column_ref, row_pot_ref, part_ref, sum_ref,
):
    half = row_pot_ref.shape[0]
    down = log_share_ref[...] - over_peers(got_ref[...])
    own = jnp.where(spot_ref[0] == 0.0, down[0], down[1])
    norm = cell_norm_ref[...]
    first = spot_ref[1] == 0.0
    row_pot_ref[...] = jnp.where(first, own[:half], own[half:]) + jnp.where(first, norm[:half], norm[half:])
    log_sums(jnp.max(safe_ref[...]) > 0.5, down, gibbs_ref, cells_ref, sites_ref, column_ref, part_ref, sum_ref, False)
    send_term(mix_ref, level_ref, column_ref, send_ref)


def last_kernel(spot_ref, terms_ref, column_ref, site_norm_ref, own_ref, other_ref):
    n_blocks = site_norm_ref.shape[0]
    log_bary = jnp.sum(terms_ref[...], axis=0)
    potential = EPS * (log_bary[None] - column_ref[...] + site_norm_ref[...][None])
    first = spot_ref[0] == 0.0
    own_ref[:n_blocks, :] = jnp.where(first, potential[0], potential[1])
    other_ref[:n_blocks, :] = jnp.where(first, potential[1], potential[0])
    own_ref[n_blocks:, :] = log_bary
    other_ref[n_blocks:, :] = log_bary


def exchange(value, axes):
    return lax.all_to_all(value, axes, split_axis=0, concat_axis=0, tiled=True)


def swapped(value, flip):
    return lax.ppermute(value, SWAP_GROUP, [(k, k ^ flip) for k in range(4)])


def on_device(demand, start_potential, cell_feat, site_feat, weights):
    n_home = lax.axis_size(HOME_GROUP)
    n_row = lax.axis_size(ROW_GROUP)
    n_bary = lax.axis_size(BARY_GROUP)
    n_sites = start_potential.shape[1] // n_home
    n_cells = demand.shape[1] * 2
    site_blocks, cell_blocks = n_sites // LANE, n_cells // LANE
    quarter = lax.axis_index(HOME_GROUP)
    place = jnp.stack([lax.axis_index(BARY_GROUP), lax.axis_index("core"), lax.axis_index("xh")]).astype(jnp.int32)

    width = cell_feat.size
    n_all = lax.axis_size(CELL_ORDER)
    (packed,) = call(pack_kernel, [((n_all, width // LANE, LANE), BF16)], cell_feat.T)
    packed, demand, start_potential = lax.optimization_barrier((packed, demand, start_potential))
    feat = exchange(packed, CELL_ORDER)
    feat = feat.reshape(n_all, width)
    core_pot = swapped(start_potential, CORE)
    own_sites = lax.dynamic_slice_in_dim(site_feat, quarter * n_sites, n_sites, 1)
    weight = weights.reshape(1, -1)
    on_cells, on_sites = (2, cell_blocks, LANE), (2, site_blocks, LANE)
    sites, site_norm, site_top, level, part, mix, share, spot = call(
        prep_kernel,
        [
            ((width, n_sites), BF16),
            ((site_blocks, LANE), F32),
            ((8, LANE), F32),
            (on_sites, F32),
            (on_sites, F32),
            ((2, 1, LANE), F32),
            ((cell_blocks // 2, LANE), F32),
            ((2, 1, LANE), F32),
        ],
        place, own_sites, in_hbm(start_potential), core_pot, in_hbm(weight), in_hbm(demand),
        scratch=[(1, n_sites), weight.shape, demand.shape, pltpu.SemaphoreType.DMA((3,))],
        apart=(2, 4, 5),
    )
    feat, sites, site_norm, site_top, level, part, mix, share, spot = lax.optimization_barrier(
        (feat, sites, site_norm, site_top, level, part, mix, share, spot)
    )
    row_outs = [((n_row, *on_cells), F32), (on_sites, F32)]
    row_scratch = [on_cells, on_sites]
    gibbs, cells, cell_norm, safe, send = call(
        build_kernel,
        [
            ((n_cells, n_sites), F32),
            ((n_cells, width), BF16),
            ((cell_blocks, LANE), F32),
            ((8, LANE), F32),
            ((n_row, 2 * cell_blocks + cell_blocks // 2, LANE), F32),
        ],
        feat, sites, site_top, level, part, share, scratch=[on_cells, (2, n_cells, LANE)], limit=24,
    )
    for repeat in range(ITERS):
        got = exchange(send, ROW_GROUP)
        column_outs = [((n_bary, site_blocks, LANE), F32), (on_sites, F32)]
        column_scratch = [on_cells, (2, site_blocks, 8, LANE)]
        if repeat == 0:
            send, column, log_share = call(
                first_column_kernel, [*column_outs, (on_cells, F32)],
                safe, mix, got, level, gibbs, cells, sites, scratch=column_scratch,
            )
        else:
            send, column, row_pot = call(
                next_column_kernel, [*column_outs, ((cell_blocks // 2, LANE), F32)],
                safe, spot, mix, log_share, got, cell_norm, level, gibbs, cells, sites, scratch=column_scratch,
            )
        terms = exchange(send, BARY_GROUP)
        if repeat < ITERS - 1:
            send, level = call(
                next_row_kernel, row_outs, safe, terms, column, gibbs, cells, sites, scratch=row_scratch
            )
    message = ((2 * site_blocks, LANE), F32)
    own, other = call(last_kernel, [message] * 2, spot, terms, column, site_norm)
    own, other, here, row_pot = lax.optimization_barrier((own, other, quarter, row_pot))
    pieces = (own, swapped(other, CORE), swapped(own, FAR), swapped(other, CROSS))
    ordered = lax.optimization_barrier(jnp.stack([lax.select_n(here ^ k, *pieces) for k in range(n_home)]))
    potential, log_bary = ordered[:, :site_blocks], ordered[:, site_blocks:]
    return EPS * row_pot.reshape(1, -1), potential.reshape(1, -1), log_bary.reshape(-1)


def solution(mesh):
    torus = Mesh(
        mesh.devices.reshape(8, 4, 2, mesh.shape["cell"], mesh.shape["site"]), ("z", "y", "core", "xh", "xl")
    )
    return jax.shard_map(
        on_device,
        mesh=torus,
        in_specs=(P(SCEN, "xh"), P(SCEN, "xl"), P(None, CELL_ORDER), P(None, "xl"), P()),
        out_specs=(P(SCEN, "xh"), P(SCEN, "xl"), P("xl")),
        check_vma=False,
    )
```

```python
import math

import jax
import jax.numpy as jnp
from jax import lax
from jax.experimental import pallas as pl
from jax.experimental.pallas import tpu as pltpu
from jax.sharding import Mesh
from jax.sharding import PartitionSpec as P

ITERS = 2
EPS = 0.25
SCEN = ("z", "y", "core")
CELL_ORDER = ("xh", "z", "y", "core", "xl")
ROW_GROUP = ("xh", "xl", "core")
BARY_GROUP = ("z", "y")
HOME_GROUP = ("xh", "core")
SWAP_GROUP = ("core", "xh")
CORE, FAR, CROSS = 2, 1, 3
F32 = jnp.float32
BF16 = jnp.bfloat16
SAFE_NORMS = 14400.0
LANE = 128
VMEM = pl.BlockSpec(memory_space=pltpu.VMEM)
SMEM = pl.BlockSpec(memory_space=pltpu.SMEM)
HBM = pl.BlockSpec(memory_space=pltpu.HBM)


def diagonal():
    shape = (LANE, LANE)
    return lax.broadcasted_iota(jnp.int32, shape, 0) == lax.broadcasted_iota(jnp.int32, shape, 1)


def to_row(column):
    return jnp.sum(jnp.where(diagonal(), column, 0.0), axis=0, keepdims=True)


def to_column(row):
    return jnp.sum(jnp.where(diagonal(), row, 0.0), axis=1, keepdims=True)


def block_at(i, size):
    return pl.ds(pl.multiple_of(i * size, size), size)


def unrolled_loop(steps, by, body):
    def several(i, _):
        for u in range(by):
            body(i * by + u)
        return 0

    lax.fori_loop(0, steps // by, several, 0)


def in_hbm(value):
    return pltpu.with_memory_space_constraint(value, pltpu.HBM)


def call(kernel, outs, *args, scratch=(), limit=16, apart=()):
    def spec(a):
        return SMEM if a.dtype == jnp.int32 else VMEM

    outs = tuple(jax.ShapeDtypeStruct(*o) for o in outs)
    return pl.pallas_call(
        kernel,
        out_shape=outs,
        in_specs=[HBM if k in apart else spec(a) for k, a in enumerate(args)],
        out_specs=tuple(spec(o) for o in outs),
        scratch_shapes=[pltpu.VMEM(s, F32) if isinstance(s, tuple) else s for s in scratch],
        compiler_params=pltpu.CompilerParams(vmem_limit_bytes=limit << 20),
    )(*args)


def pack_kernel(feat_ref, out_ref):
    per_row, depth = feat_ref.shape
    width = depth * per_row
    spread = lax.broadcasted_iota(jnp.int32, (depth, width), 1) // per_row == lax.broadcasted_iota(
        jnp.int32, (depth, width), 0
    )
    wide = jnp.dot(feat_ref[...], jnp.where(spread, 1.0, 0.0).astype(BF16), preferred_element_type=F32)
    own = lax.broadcasted_iota(jnp.int32, (per_row, width), 1) % per_row == lax.broadcasted_iota(
        jnp.int32, (per_row, width), 0
    )
    line = jnp.sum(jnp.where(own, wide, 0.0), axis=0, keepdims=True)
    lines = jnp.concatenate([line[:, h * LANE : (h + 1) * LANE] for h in range(width // LANE)], axis=0)
    out_ref[...] = jnp.broadcast_to(lines.astype(BF16)[None], out_ref.shape)


def prep_kernel(
    place_ref, site_ref, pot_ref, core_pot_ref, weight_ref, demand_ref,
    sites_ref, site_norm_ref, site_top_ref, level_ref, part_ref, mix_ref, share_ref, spot_ref,
    quarter_ref, weights_ref, line_ref, sems,
):
    width = sites_ref.shape[0]
    depth, n_sites = site_ref.shape
    core, far = place_ref[1], place_ref[2]
    here = pl.ds(pl.multiple_of((2 * far + core) * n_sites, n_sites), n_sites)
    copies = [
        pltpu.make_async_copy(pot_ref.at[:, here], quarter_ref, sems.at[0]),
        pltpu.make_async_copy(weight_ref, weights_ref, sems.at[1]),
        pltpu.make_async_copy(demand_ref, line_ref, sems.at[2]),
    ]
    for copy in copies:
        copy.start()
    site = site_ref[...]
    wide = site.astype(F32)
    site_norm = jnp.sum(wide * wide, axis=0, keepdims=True)
    site_top_ref[...] = jnp.broadcast_to(jnp.max(site_norm, axis=1, keepdims=True), site_top_ref.shape)
    for b in range(n_sites // LANE):
        site_norm_ref[b : b + 1, :] = site_norm[:, b * LANE : (b + 1) * LANE] / (depth * EPS)
    spread = (
        lax.broadcasted_iota(jnp.int32, (width, depth), 0) // (width // depth)
        == lax.broadcasted_iota(jnp.int32, (width, depth), 1)
    )
    sites_ref[...] = jnp.dot(
        jnp.where(spread, 1.0, 0.0).astype(BF16), site, preferred_element_type=F32
    ).astype(BF16)
    for copy in copies:
        copy.wait()
    for s, line in enumerate(by_core(core, quarter_ref[...], core_pot_ref[:, here])):
        for b in range(n_sites // LANE):
            level_ref[s, b : b + 1, :] = line[:, b * LANE : (b + 1) * LANE]
    level = level_ref[...] * (1.0 / EPS) - site_norm_ref[...][None]
    level_ref[...] = level
    part_ref[...] = jnp.exp(level - overall(jnp.max, level))
    for k, bit in enumerate((core, far)):
        spot_ref[k] = jnp.full(spot_ref.shape[1:], bit, jnp.int32).astype(F32)
    for b in range(share_ref.shape[0]):
        share_ref[b : b + 1, :] = line_ref[:, b * LANE : (b + 1) * LANE]
    weight = weights_ref[...]
    which = lax.broadcasted_iota(jnp.int32, weight.shape, 1)
    total = jnp.sum(weight, axis=1, keepdims=True)
    for s in range(2):
        own = jnp.sum(jnp.where(which == 2 * place_ref[0] + s, weight, 0.0), axis=1, keepdims=True)
        mix_ref[s] = jnp.broadcast_to(own / total, mix_ref.shape[1:])


def by_core(core, own, other):
    return jnp.where(core == 0, own, other), jnp.where(core == 0, other, own)


def overall(reduce, value):
    return reduce(reduce(value, axis=2, keepdims=True), axis=1, keepdims=True)


def cell_rows(i, feat, size, per_row):
    width = feat.shape[1]
    rows = lax.broadcasted_iota(jnp.int32, (size, width), 0)
    lanes = lax.broadcasted_iota(jnp.int32, (size, width), 1)
    pick = jnp.where(rows // per_row + i * (size // per_row) == lanes, 1.0, 0.0).astype(BF16)
    block = jnp.dot(pick, feat, preferred_element_type=F32)
    return jnp.where(rows % per_row == lanes % per_row, block, 0.0).astype(BF16)


def build_kernel(
    feat_ref, sites_ref, site_top_ref, level_ref, part_ref, share_ref,
    gibbs_ref, cells_ref, cell_norm_ref, safe_ref, send_ref, out_ref, sum_ref,
):
    n_cells, width = cells_ref.shape
    n_sites = sites_ref.shape[1]
    n_lines = feat_ref.shape[0]
    per_row = n_cells // n_lines
    depth = width // per_row
    rows_blk, cols_blk = 2048, 512
    feat = feat_ref[...]
    wide = feat.astype(F32)
    square = wide * wide
    high = square.astype(BF16)
    low = (square - high.astype(F32)).astype(BF16)
    same = lax.broadcasted_iota(jnp.int32, (width, LANE), 0) % per_row == lax.broadcasted_iota(
        jnp.int32, (width, LANE), 1
    ) % per_row
    fold = jnp.where(same, 1.0, 0.0).astype(BF16)
    norm = jnp.dot(high, fold, preferred_element_type=F32) + jnp.dot(low, fold, preferred_element_type=F32)
    group = LANE // per_row
    own = lax.broadcasted_iota(jnp.int32, (n_lines, LANE), 0) % group == lax.broadcasted_iota(
        jnp.int32, (n_lines, LANE), 1
    ) // per_row
    cell_norm_ref[...] = jnp.sum(
        jnp.where(own, norm, 0.0).reshape(n_cells // LANE, group, LANE), axis=1
    ) / (depth * EPS)
    safe = jnp.max(norm) * jnp.max(site_top_ref[...]) <= SAFE_NORMS
    safe_ref[...] = jnp.full(safe_ref.shape, jnp.where(safe, 1.0, 0.0), F32)

    @pl.when(safe)
    def _():
        scale = 2.0 / (depth * EPS) * math.log2(math.e)

        def block(i):
            at = block_at(i, rows_blk)
            rows = cell_rows(i, feat_ref[...], rows_blk, per_row)
            for j in range(n_sites // cols_blk):
                inner = jnp.dot(
                    rows, sites_ref[:, j * cols_blk : (j + 1) * cols_blk], preferred_element_type=F32
                )
                values = jnp.exp2(inner * scale)
                gibbs_ref[at, j * cols_blk : (j + 1) * cols_blk] = values
                for s in range(2):
                    terms = [
                        values[:, b * LANE : (b + 1) * LANE]
                        * part_ref[s, j * (cols_blk // LANE) + b : j * (cols_blk // LANE) + b + 1, :]
                        for b in range(cols_blk // LANE)
                    ]
                    added = (terms[0] + terms[1]) + (terms[2] + terms[3])
                    if j == 0:
                        sum_ref[s, at, :] = added
                    else:
                        sum_ref[s, at, :] += added

        unrolled_loop(n_cells // rows_blk, 1, block)

        def fold_block(i):
            at = block_at(i, LANE)
            for s in range(2):
                out_ref[s, pl.ds(i, 1), :] = to_row(jnp.sum(sum_ref[s, at, :], axis=1, keepdims=True))

        unrolled_loop(n_cells // LANE, 16, fold_block)
        out_ref[...] = overall(jnp.max, level_ref[...]) + jnp.log(out_ref[...])

    @pl.when(jnp.logical_not(safe))
    def _():
        for i in range(n_cells // rows_blk):
            cells_ref[i * rows_blk : (i + 1) * rows_blk, :] = cell_rows(i, feat_ref[...], rows_blk, per_row)
        log_domain(level_ref[...], cells_ref, sites_ref, out_ref, True)

    flat = out_ref.shape[0] * out_ref.shape[1]
    send_ref[:, :flat, :] = jnp.broadcast_to(out_ref[...].reshape(1, flat, LANE), (send_ref.shape[0], flat, LANE))
    send_ref[:, flat:, :] = jnp.broadcast_to(share_ref[...][None], (send_ref.shape[0], *share_ref.shape))


def log_domain(level, cells_ref, sites_ref, out_ref, over_sites):
    n_scen, blocks_in, _ = level.shape
    scale = 2.0 / ((cells_ref.shape[1] // 8) * EPS)

    def block(i, _):
        at = block_at(i, LANE)
        if over_sites:
            inner = jnp.dot(cells_ref[at, :], sites_ref[...], preferred_element_type=F32)
        else:
            inner = lax.dot_general(
                sites_ref[:, at], cells_ref[...], (((0,), (1,)), ((), ())), preferred_element_type=F32
            )
        for s in range(n_scen):
            score = inner * scale + jnp.concatenate([level[s, b : b + 1, :] for b in range(blocks_in)], axis=1)
            top = jnp.max(score, axis=1, keepdims=True)
            total = jnp.sum(jnp.exp(score - top), axis=1, keepdims=True)
            out_ref[s, pl.ds(i, 1), :] = to_row(top + jnp.log(total))
        return 0

    lax.fori_loop(0, out_ref.shape[1], block, 0)


def log_sums(safe, level, gibbs_ref, cells_ref, sites_ref, out_ref, part_ref, sum_ref, over_sites):
    n_scen, blocks_in, _ = level.shape
    blocks_out = out_ref.shape[1]

    @pl.when(safe)
    def _():
        top = overall(jnp.max, level)
        part_ref[...] = jnp.exp(level - top)
        if over_sites:

            def cell_block(i):
                at = block_at(i, LANE)
                sums = [jnp.zeros((LANE, LANE), F32) for _ in range(n_scen)]
                for b in range(blocks_in):
                    tile = gibbs_ref[at, b * LANE : (b + 1) * LANE]
                    for s in range(n_scen):
                        sums[s] += tile * part_ref[s, b : b + 1, :]
                for s in range(n_scen):
                    out_ref[s, pl.ds(i, 1), :] = to_row(jnp.sum(sums[s], axis=1, keepdims=True))

            unrolled_loop(blocks_out, 16, cell_block)
        else:
            sum_ref[...] = jnp.zeros_like(sum_ref)

            def cell_block(i):
                at = block_at(i, LANE)
                columns = [
                    jnp.broadcast_to(to_column(part_ref[s, pl.ds(i, 1), :]), (LANE, LANE)) for s in range(n_scen)
                ]
                for b in range(blocks_out):
                    tile = gibbs_ref[at, b * LANE : (b + 1) * LANE]
                    for s in range(n_scen):
                        sum_ref[s, b] += jnp.sum((tile * columns[s]).reshape(LANE // 8, 8, LANE), axis=0)

            unrolled_loop(blocks_in, 16, cell_block)
            out_ref[...] = jnp.sum(sum_ref[...], axis=2)
        out_ref[...] = top + jnp.log(out_ref[...])

    @pl.when(jnp.logical_not(safe))
    def _():
        log_domain(level, cells_ref, sites_ref, out_ref, over_sites)


def next_row_kernel(
    safe_ref, terms_ref, column_ref, gibbs_ref, cells_ref, sites_ref, send_ref, level_ref, out_ref, part_ref
):
    level = jnp.sum(terms_ref[...], axis=0)[None] - column_ref[...]
    level_ref[...] = level
    log_sums(jnp.max(safe_ref[...]) > 0.5, level, gibbs_ref, cells_ref, sites_ref, out_ref, part_ref, None, True)
    send_ref[...] = jnp.broadcast_to(out_ref[...][None], send_ref.shape)


def over_peers(got):
    top = jnp.max(got, axis=0)
    return top + jnp.log(jnp.sum(jnp.exp(got - top[None]), axis=0))


def send_term(mix_ref, level_ref, column_ref, send_ref):
    term = mix_ref[0] * (level_ref[0] + column_ref[0]) + mix_ref[1] * (level_ref[1] + column_ref[1])
    send_ref[...] = jnp.broadcast_to(term[None], send_ref.shape)


def first_column_kernel(
    safe_ref, mix_ref, got_ref, level_ref, gibbs_ref, cells_ref, sites_ref,
    send_ref, column_ref, log_share_ref, part_ref, sum_ref,
):
    on_cells = log_share_ref.shape
    flat = on_cells[0] * on_cells[1]
    near, away = 0, got_ref.shape[0] // 2
    for s in range(2):
        log_share_ref[s] = jnp.concatenate([got_ref[near + s, flat:, :], got_ref[away + s, flat:, :]], axis=0)
    demand = log_share_ref[...]
    log_share = jnp.log(demand) - jnp.log(overall(jnp.sum, demand))
    log_share_ref[...] = log_share
    down = log_share - over_peers(got_ref[:, :flat, :]).reshape(on_cells)
    log_sums(jnp.max(safe_ref[...]) > 0.5, down, gibbs_ref, cells_ref, sites_ref, column_ref, part_ref, sum_ref, False)
    send_term(mix_ref, level_ref, column_ref, send_ref)


def next_column_kernel(
    safe_ref, spot_ref, mix_ref, log_share_ref, got_ref, cell_norm_ref, level_ref, gibbs_ref, cells_ref, sites_ref,
    send_ref, column_ref, row_pot_ref, part_ref, sum_ref,
):
    half = row_pot_ref.shape[0]
    down = log_share_ref[...] - over_peers(got_ref[...])
    own = jnp.where(spot_ref[0] == 0.0, down[0], down[1])
    norm = cell_norm_ref[...]
    first = spot_ref[1] == 0.0
    row_pot_ref[...] = jnp.where(first, own[:half], own[half:]) + jnp.where(first, norm[:half], norm[half:])
    log_sums(jnp.max(safe_ref[...]) > 0.5, down, gibbs_ref, cells_ref, sites_ref, column_ref, part_ref, sum_ref, False)
    send_term(mix_ref, level_ref, column_ref, send_ref)


def last_kernel(spot_ref, terms_ref, column_ref, site_norm_ref, own_ref, other_ref):
    n_blocks = site_norm_ref.shape[0]
    log_bary = jnp.sum(terms_ref[...], axis=0)
    potential = EPS * (log_bary[None] - column_ref[...] + site_norm_ref[...][None])
    first = spot_ref[0] == 0.0
    own_ref[:n_blocks, :] = jnp.where(first, potential[0], potential[1])
    other_ref[:n_blocks, :] = jnp.where(first, potential[1], potential[0])
    own_ref[n_blocks:, :] = log_bary
    other_ref[n_blocks:, :] = log_bary


def exchange(value, axes):
    return lax.all_to_all(value, axes, split_axis=0, concat_axis=0, tiled=True)


def swapped(value, flip):
    return lax.ppermute(value, SWAP_GROUP, [(k, k ^ flip) for k in range(4)])


def on_device(demand, start_potential, cell_feat, site_feat, weights):
    n_home = lax.axis_size(HOME_GROUP)
    n_row = lax.axis_size(ROW_GROUP)
    n_bary = lax.axis_size(BARY_GROUP)
    n_sites = start_potential.shape[1] // n_home
    n_cells = demand.shape[1] * 2
    site_blocks, cell_blocks = n_sites // LANE, n_cells // LANE
    quarter = lax.axis_index(HOME_GROUP)
    place = jnp.stack([lax.axis_index(BARY_GROUP), lax.axis_index("core"), lax.axis_index("xh")]).astype(jnp.int32)

    width = cell_feat.size
    n_all = lax.axis_size(CELL_ORDER)
    (packed,) = call(pack_kernel, [((n_all, width // LANE, LANE), BF16)], cell_feat.T)
    packed, demand, start_potential = lax.optimization_barrier((packed, demand, start_potential))
    feat = exchange(packed, CELL_ORDER)
    feat = feat.reshape(n_all, width)
    core_pot = swapped(start_potential, CORE)
    own_sites = lax.dynamic_slice_in_dim(site_feat, quarter * n_sites, n_sites, 1)
    weight = weights.reshape(1, -1)
    on_cells, on_sites = (2, cell_blocks, LANE), (2, site_blocks, LANE)
    sites, site_norm, site_top, level, part, mix, share, spot = call(
        prep_kernel,
        [
            ((width, n_sites), BF16),
            ((site_blocks, LANE), F32),
            ((8, LANE), F32),
            (on_sites, F32),
            (on_sites, F32),
            ((2, 1, LANE), F32),
            ((cell_blocks // 2, LANE), F32),
            ((2, 1, LANE), F32),
        ],
        place, own_sites, in_hbm(start_potential), core_pot, in_hbm(weight), in_hbm(demand),
        scratch=[(1, n_sites), weight.shape, demand.shape, pltpu.SemaphoreType.DMA((3,))],
        apart=(2, 4, 5),
    )
    feat, sites, site_norm, site_top, level, part, mix, share, spot = lax.optimization_barrier(
        (feat, sites, site_norm, site_top, level, part, mix, share, spot)
    )
    row_outs = [((n_row, *on_cells), F32), (on_sites, F32)]
    row_scratch = [on_cells, on_sites]
    gibbs, cells, cell_norm, safe, send = call(
        build_kernel,
        [
            ((n_cells, n_sites), F32),
            ((n_cells, width), BF16),
            ((cell_blocks, LANE), F32),
            ((8, LANE), F32),
            ((n_row, 2 * cell_blocks + cell_blocks // 2, LANE), F32),
        ],
        feat, sites, site_top, level, part, share, scratch=[on_cells, (2, n_cells, LANE)], limit=24,
    )
    for repeat in range(ITERS):
        got = exchange(send, ROW_GROUP)
        column_outs = [((n_bary, site_blocks, LANE), F32), (on_sites, F32)]
        column_scratch = [on_cells, (2, site_blocks, 8, LANE)]
        if repeat == 0:
            send, column, log_share = call(
                first_column_kernel, [*column_outs, (on_cells, F32)],
                safe, mix, got, level, gibbs, cells, sites, scratch=column_scratch,
            )
        else:
            send, column, row_pot = call(
                next_column_kernel, [*column_outs, ((cell_blocks // 2, LANE), F32)],
                safe, spot, mix, log_share, got, cell_norm, level, gibbs, cells, sites, scratch=column_scratch,
            )
        terms = exchange(send, BARY_GROUP)
        if repeat < ITERS - 1:
            send, level = call(
                next_row_kernel, row_outs, safe, terms, column, gibbs, cells, sites, scratch=row_scratch
            )
    message = ((2 * site_blocks, LANE), F32)
    own, other = call(last_kernel, [message] * 2, spot, terms, column, site_norm)
    own, other, here, row_pot = lax.optimization_barrier((own, other, quarter, row_pot))
    pieces = (own, swapped(other, CORE), swapped(own, FAR), swapped(other, CROSS))
    ordered = lax.optimization_barrier(jnp.stack([lax.select_n(here ^ k, *pieces) for k in range(n_home)]))
    potential, log_bary = ordered[:, :site_blocks], ordered[:, site_blocks:]
    return EPS * row_pot.reshape(1, -1), potential.reshape(1, -1), log_bary.reshape(-1)


def solution(mesh):
    torus = Mesh(
        mesh.devices.reshape(8, 4, 2, mesh.shape["cell"], mesh.shape["site"]), ("z", "y", "core", "xh", "xl")
    )
    return jax.shard_map(
        on_device,
        mesh=torus,
        in_specs=(P(SCEN, "xh"), P(SCEN, "xl"), P(None, CELL_ORDER), P(None, "xl"), P()),
        out_specs=(P(SCEN, "xh"), P(SCEN, "xl"), P("xl")),
        check_vma=False,
    )
```
